32 devices in a mesh: batch: 8 (over z, x), cols: 4 (over y, core).
Axes of the slice: x: 2, y: 2, z: 4, core: 2. Of those that a mesh axis runs over, the one named last changes fastest.
Arguments:
- partial_query: float32 [8, 1024, 1024], P('batch', None, 'cols'), may hold values from -0.875 to 0.875
- partial_key: float32 [8, 1024, 1024], P('batch', None, 'cols'), may hold values from -0.875 to 0.875
- partial_value: float32 [8, 1024, 1024], P('batch', None, 'cols'), may hold values from -0.875 to 0.875
- partial_mixed: float32 [8, 1024, 1024], P('batch', 'cols'), may hold values from -0.875 to 0.875
- partial_norm: float32 [8, 1024], P('batch'), may hold values from -8 to 8
- partial_bias: float32 [8, 1024], P('batch'), may hold values from -8 to 8
- master_query: float32 [1024, 1024], P('batch', 'cols'), may hold values from -0.1875 to 0.1875
- master_key: float32 [1024, 1024], P('batch', 'cols'), may hold values from -0.1875 to 0.1875
- master_value: float32 [1024, 1024], P('batch', 'cols'), may hold values from -0.1875 to 0.1875
- master_mixed: float32 [1024, 1024], P('cols', 'batch'), may hold values from -0.1875 to 0.1875
- master_norm: float32 [1024], P('batch'), may hold values from 0.25 to 1.75
- master_bias: float32 [1024], P('batch'), may hold values from -3 to 3
Outputs:
- compute_query: bfloat16 [1024, 1024], P(None, 'cols')
- compute_key: bfloat16 [1024, 1024], P(None, 'cols')
- compute_value: bfloat16 [1024, 1024], P(None, 'cols')
- compute_mixed: bfloat16 [1024, 1024], P('cols')
- compute_norm: bfloat16 [1024], replicated
- compute_bias: bfloat16 [1024], replicated
- stepped_query: float32 [1024, 1024], P('batch', 'cols')
- stepped_key: float32 [1024, 1024], P('batch', 'cols')
- stepped_value: float32 [1024, 1024], P('batch', 'cols')
- stepped_mixed: float32 [1024, 1024], P('cols', 'batch')
- stepped_norm: float32 [1024], P('batch')
- stepped_bias: float32 [1024], P('batch')
The draws below stay inside these ranges and needn't reach their ends.
All inputs are finite; a program needn't handle non-finite values.
Results may differ from the reference program's by a relative error of at most 0.001.
Values may be sent and summed in bfloat16 or wider, within the bound.
A program may use at most 64 MiB of HBM per device.

```python
import jax
import jax.numpy as jnp

WIDTH = 1024
ATTN = 1024
REPLICAS = 8


def with_spikes(array, stream_key, source, target, blocks, factor):
    owner, partner = [(jnp.arange(array.shape[axis_at]) // (array.shape[axis_at] // blocks)).reshape([-1 if axis == axis_at else 1 for axis in range(array.ndim)]) for axis_at in (source, target)]
    chosen = jax.random.permutation(stream_key, blocks)[partner]
    strong = (owner == chosen) | (owner == (partner + blocks // 2) % blocks)
    return jnp.where(strong, factor * array, array)


def levels(rng, extent, cuts, smallest, top_value):
    def one(position, blocks):
        heights = jax.random.uniform(jax.random.fold_in(jax.random.fold_in(rng, 6), position), (blocks,), jnp.float32, smallest / len(cuts), top_value / len(cuts))
        return jnp.repeat(jnp.exp(heights), extent[position] // blocks).reshape((-1,) + (1,) * (len(extent) - position - 1))

    loudness = one(*cuts[0])
    for cut in cuts[1:]:
        loudness = loudness * one(*cut)
    return loudness


def gaussian(stream_key, extent, spread, limit, shards=(), dtype=jnp.bfloat16):
    loudness = levels(stream_key, extent, shards, -0.22, 0.18) if shards else 1.0
    drawn = jax.random.normal(stream_key, extent, jnp.float32) * spread * loudness
    return jnp.minimum(jnp.maximum(drawn, -limit), limit).astype(dtype)


def heavy_noise(stream_key, dims, deviation, reach, cuts, heavy, kind=jnp.bfloat16):
    drawn = deviation * jax.random.normal(stream_key, dims, jnp.float32)
    if cuts:
        drawn = drawn * levels(stream_key, dims, cuts, -0.22, 0.18)
    return jnp.clip(with_spikes(drawn, jax.random.fold_in(stream_key, 3), *heavy), -reach, reach).astype(kind)


def setup_inputs(seed: int = 0) -> dict:
    splits = jax.random.split(jax.random.key(seed), 13)
    partial_query = heavy_noise(splits[0], (REPLICAS, WIDTH, ATTN), 0.1, 0.875, ((0, 8), (2, 4)), (0, 1, 8, 2.0), jnp.float32)
    partial_key = heavy_noise(splits[1], (REPLICAS, WIDTH, ATTN), 0.1, 0.875, ((0, 8), (2, 4)), (0, 1, 8, 2.0), jnp.float32)
    partial_value = heavy_noise(splits[2], (REPLICAS, WIDTH, ATTN), 0.1, 0.875, ((0, 8), (2, 4)), (0, 1, 8, 2.0), jnp.float32)
    partial_mixed = heavy_noise(splits[3], (REPLICAS, ATTN, WIDTH), 0.1, 0.875, ((0, 8), (1, 4)), (0, 2, 8, 2.0), jnp.float32)
    partial_norm = heavy_noise(splits[4], (REPLICAS, WIDTH), 1.0, 8.0, ((0, 8),), (0, 1, 8, 2.0), jnp.float32)
    partial_bias = heavy_noise(splits[5], (REPLICAS, WIDTH), 1.0, 8.0, ((0, 8),), (0, 1, 8, 2.0), jnp.float32)
    master_query = gaussian(splits[6], (WIDTH, ATTN), WIDTH ** -0.5, 0.1875, ((0, 8), (1, 4)), jnp.float32)
    master_key = gaussian(splits[7], (WIDTH, ATTN), WIDTH ** -0.5, 0.1875, ((0, 8), (1, 4)), jnp.float32)
    master_value = gaussian(splits[8], (WIDTH, ATTN), WIDTH ** -0.5, 0.1875, ((0, 8), (1, 4)), jnp.float32)
    master_mixed = gaussian(splits[9], (ATTN, WIDTH), ATTN ** -0.5, 0.1875, ((0, 4), (1, 8)), jnp.float32)
    master_norm = jnp.clip(1.0 + 0.15 * jax.random.normal(splits[10], (WIDTH,), jnp.float32), 0.25, 1.75)
    master_bias = gaussian(splits[11], (WIDTH,), 0.5, 3.0, ((0, 8),), jnp.float32)
    return {"partial_query": partial_query, "partial_key": partial_key, "partial_value": partial_value, "partial_mixed": partial_mixed, "partial_norm": partial_norm, "partial_bias": partial_bias, "master_query": master_query, "master_key": master_key, "master_value": master_value, "master_mixed": master_mixed, "master_norm": master_norm, "master_bias": master_bias}


learn_rate = 0.4


def reference(partial_query, partial_key, partial_value, partial_mixed, partial_norm, partial_bias, master_query, master_key, master_value, master_mixed, master_norm, master_bias):
    mean_query = jnp.sum(partial_query.astype(jnp.float32), axis=0) * REPLICAS ** -0.5
    mean_key = jnp.sum(partial_key.astype(jnp.float32), axis=0) * REPLICAS ** -0.5
    mean_value = jnp.sum(partial_value.astype(jnp.float32), axis=0) * REPLICAS ** -0.5
    mean_mixed = jnp.sum(partial_mixed.astype(jnp.float32), axis=0) * REPLICAS ** -0.5
    mean_norm = jnp.sum(partial_norm.astype(jnp.float32), axis=0) * REPLICAS ** -0.5
    mean_bias = jnp.sum(partial_bias.astype(jnp.float32), axis=0) * REPLICAS ** -0.5
    stepped_query = master_query - learn_rate * mean_query
    stepped_key = master_key - learn_rate * mean_key
    stepped_value = master_value - learn_rate * mean_value
    stepped_mixed = master_mixed - learn_rate * mean_mixed
    stepped_norm = master_norm - learn_rate * mean_norm
    stepped_bias = master_bias - learn_rate * mean_bias
    compute_query = stepped_query.astype(jnp.bfloat16)
    compute_key = stepped_key.astype(jnp.bfloat16)
    compute_value = stepped_value.astype(jnp.bfloat16)
    compute_mixed = stepped_mixed.astype(jnp.bfloat16)
    compute_norm = stepped_norm.astype(jnp.bfloat16)
    compute_bias = stepped_bias.astype(jnp.bfloat16)
    return compute_query, compute_key, compute_value, compute_mixed, compute_norm, compute_bias, stepped_query, stepped_key, stepped_value, stepped_mixed, stepped_norm, stepped_bias
```

```python
import functools

import jax
import jax.numpy as jnp
from jax import lax
from jax.experimental import pallas as pl
from jax.experimental.pallas import tpu as pltpu
from jax.sharding import PartitionSpec as P

learn_rate = 0.4
HALVES = 2
SPAN = 118.0


def encode(x, limit):
    power = jnp.exp2(jnp.abs(x) * (2 * SPAN / limit) - SPAN)
    return jnp.where(x < 0, -power, power).astype(jnp.bfloat16)


def decode(code, limit):
    y = code.astype(jnp.float32)
    size = (jnp.log2(jnp.abs(y)) + SPAN) * (limit / (2 * SPAN))
    return jnp.where(y < 0, -size, size)


def kernel(n, kinds, limit, *refs):
    count = len(kinds)
    groups = n // 2
    refs = list(refs)

    def take(k):
        out = refs[:k]
        del refs[:k]
        return out

    source, master = take(count), take(count)
    norm, bias, norm_master, bias_master = take(4)
    gathered, stepped = take(count), take(count)
    vec_all, vec_mine = take(2)
    pair_out, pair_in, part_out, part_in = take(count), take(count), take(count), take(count)
    own, partial = take(count), take(count)
    vec_out, vec_in = take(2)
    (in_sem,) = take(1)
    a_send, a_recv, b_send, b_recv, c_send, c_recv, d_send, d_recv = take(8)
    v_send, v_recv, w_send, w_recv = take(4)

    rate = n ** (-0.5)
    b = lax.axis_index("batch")
    side = lax.rem(b, 2)
    g = b // 2
    partner = b + 1 - 2 * side

    def remote(src, dst, send, recv, to):
        return pltpu.make_async_remote_copy(
            src_ref=src,
            dst_ref=dst,
            send_sem=send,
            recv_sem=recv,
            device_id={"batch": to},
            device_id_type=pl.DeviceIdType.MESH,
        )

    chunks = [(a, h) for h in range(HALVES) for a in range(count)]

    def place(a, h, d):
        rows, cols = stepped[a].shape
        r = rows // HALVES
        if kinds[a] == "rows":
            return pl.ds(pl.multiple_of(d * rows + h * r, r), r), pl.ds(0, cols)
        return pl.ds(h * r, r), pl.ds(pl.multiple_of(d * cols, cols), cols)

    def load(a, h, d):
        rows, cols = place(a, h, d)
        return partial[a][rows, cols]

    def other(k):
        return lax.rem(g + k, groups)

    loads = [
        pltpu.make_async_copy(source[a].at[0], partial[a], in_sem.at[a])
        for a in range(count)
    ]
    for copy in loads:
        copy.start()

    barrier = pltpu.get_barrier_semaphore()
    for k in range(1, n):
        pl.semaphore_signal(
            barrier,
            inc=1,
            device_id={"batch": lax.rem(b + k, n)},
            device_id_type=pl.DeviceIdType.MESH,
        )

    def pair_encode(c):
        a, h = chunks[c]

        def body(k, carry):
            pair_out[a][h, k] = encode(load(a, h, 2 * k + 1 - side), limit)
            return carry

        lax.fori_loop(0, groups, body, 0)

    def pair_copy(c):
        a, h = chunks[c]
        return remote(
            pair_out[a].at[h], pair_in[a].at[h], a_send.at[c], a_recv.at[c], partner
        )

    def part_copy(c, src_slot, dst_slot, to):
        a, h = chunks[c]
        return remote(
            part_out[a].at[h, src_slot],
            part_in[a].at[h, dst_slot],
            b_send.at[c, src_slot],
            b_recv.at[c, dst_slot],
            2 * to + side,
        )

    def pair_finish(c):
        a, h = chunks[c]
        pair_copy(c).wait_recv()
        for k in range(1, groups):
            to = other(k)
            total = load(a, h, 2 * to + side) + decode(pair_in[a][h, to], limit)
            part_out[a][h, to] = encode(total, 2 * limit)
            part_copy(c, to, g, to).start()
        own[a][h] = load(a, h, b) + decode(pair_in[a][h, g], limit)

    def line_copy(c, owner, way, to=None):
        a, h = chunks[c]
        rows, cols = place(a, h, owner)
        block = gathered[a].at[rows, cols]
        return remote(
            block,
            block,
            c_send.at[(way + 1) // 2, c, owner // 2],
            c_recv.at[c, owner // 2],
            b + 2 * way if to is None else to,
        )

    def has_next(way):
        return g < groups - 1 if way > 0 else g > 0

    def has_source(way, k):
        return g - k >= 0 if way > 0 else g + k < groups

    def cross_copy(c, owner, recv_owner):
        a, h = chunks[c]
        rows, cols = place(a, h, owner)
        block = gathered[a].at[rows, cols]
        return remote(
            block, block, d_send.at[c, owner // 2], d_recv.at[c, recv_owner // 2], partner
        )

    def part_finish(c):
        a, h = chunks[c]
        r = stepped[a].shape[0] // HALVES
        total = own[a][h]
        for k in range(1, groups):
            source = other(k)
            part_copy(c, source, source, source).wait_recv()
            total = total + decode(part_in[a][h, source], 2 * limit)
        rows = pl.ds(h * r, r)
        new = master[a][rows, :] - learn_rate * (total * rate)
        stepped[a][rows, :] = new
        at_rows, at_cols = place(a, h, b)
        gathered[a][at_rows, at_cols] = new.astype(jnp.bfloat16)
        for way in (1, -1):

            @pl.when(has_next(way))
            def _():
                line_copy(c, b, way).start()

        cross_copy(c, b, b).start()

    def line_finish(c, k):
        for way in (1, -1):

            @pl.when(has_source(way, k))
            def _():
                owner = b - 2 * k * way
                line_copy(c, owner, way, owner).wait_recv()

                @pl.when(has_next(way))
                def _():
                    line_copy(c, owner, way).start()

                cross_copy(c, owner, owner).start()

    def vec_copy(k):
        to = lax.rem(b + k, n)
        return remote(vec_out.at[to], vec_in.at[b], v_send.at[to], v_recv.at[b], to)

    def vec_back(k):
        to = lax.rem(b + k, n)
        return remote(vec_all.at[b], vec_all.at[b], w_send.at[to], w_recv.at[b], to)

    loads[0].wait()
    pair_encode(0)
    pl.semaphore_wait(barrier, n - 1)
    pair_copy(0).start()
    for d in range(n):
        vec_out[d, 0:1, :] = norm[d]
        vec_out[d, 1:2, :] = bias[d]
    for k in range(1, n):
        vec_copy(k).start()
    for c in range(1, len(chunks)):
        if c < count:
            loads[c].wait()
        pair_encode(c)
        pair_copy(c).start()

    for t in range(len(chunks) + groups):
        if t < len(chunks):
            pair_finish(t)
        if 0 <= t - 1 < len(chunks):
            part_finish(t - 1)
        if t == 1:
            total = vec_out[b]
            for k in range(1, n):
                source = lax.rem(b + k, n)
                remote(
                    vec_out.at[source],
                    vec_in.at[source],
                    v_send.at[source],
                    v_recv.at[source],
                    source,
                ).wait_recv()
                total = total + vec_in[source]
            mean = total * rate
            vec_mine[0:1, :] = norm_master[...] - learn_rate * mean[0:1]
            vec_mine[1:2, :] = bias_master[...] - learn_rate * mean[1:2]
            vec_all[b] = vec_mine[...]
            for k in range(1, n):
                vec_back(k).start()
        for k in range(groups - 1, 0, -1):
            if 0 <= t - 1 - k < len(chunks):
                line_finish(t - 1 - k, k)

    for c in range(len(chunks)):
        for k in range(groups):
            owner = 2 * other(k) + 1 - side
            cross_copy(c, owner, owner).wait_recv()
    for k in range(1, n):
        source = lax.rem(b + k, n)
        remote(
            vec_all.at[source],
            vec_all.at[source],
            w_send.at[source],
            w_recv.at[source],
            source,
        ).wait_recv()
    for k in range(1, n):
        vec_copy(k).wait_send()
        vec_back(k).wait_send()
    for c in range(len(chunks)):
        pair_copy(c).wait_send()
        for k in range(1, groups):
            to = other(k)
            part_copy(c, to, g, to).wait_send()
        for k in range(groups):
            owner = 2 * other(k) + side
            cross_copy(c, owner, owner).wait_send()
        for way in (1, -1):

            @pl.when(has_next(way))
            def _():
                line_copy(c, b, way).wait_send()

            for k in range(1, groups):

                @pl.when(has_source(way, k) & has_next(way))
                def _():
                    line_copy(c, b - 2 * k * way, way).wait_send()


def hand_over(count, *refs):
    sources, vec_all, vec_mine = refs[:count], refs[count], refs[count + 1]
    targets = refs[count + 2 : 2 * count + 2]
    norm, bias, norm_step, bias_step = refs[2 * count + 2 : 2 * count + 6]
    (out_sem,) = refs[2 * count + 6 :]
    outs = [
        pltpu.make_async_copy(sources[i], targets[i], out_sem.at[i]) for i in range(count)
    ]
    for copy in outs:
        copy.start()
    norm[...] = vec_all[:, 0, :].astype(jnp.bfloat16)
    bias[...] = vec_all[:, 1, :].astype(jnp.bfloat16)
    norm_step[...] = vec_mine[0:1, :]
    bias_step[...] = vec_mine[1:2, :]
    for copy in outs:
        copy.wait()


def per_device(
    partial_query,
    partial_key,
    partial_value,
    partial_mixed,
    partial_norm,
    partial_bias,
    master_query,
    master_key,
    master_value,
    master_mixed,
    master_norm,
    master_bias,
):
    n = lax.axis_size("batch")
    groups = n // 2
    limit = 0.875 if n <= 8 else 1.25
    wide = master_mixed.shape[1] % 128 == 0
    kinds = ("rows", "rows", "rows", "cols" if wide else "rows")
    if not wide:
        partial_mixed = jnp.swapaxes(partial_mixed, 1, 2)
        master_mixed = master_mixed.T
    partials = (partial_query, partial_key, partial_value, partial_mixed)
    masters = (master_query, master_key, master_value, master_mixed)
    chunk_count = len(partials) * HALVES
    w = master_norm.shape[0]

    out_shape = [jax.ShapeDtypeStruct(p.shape[1:], jnp.bfloat16) for p in partials]
    out_shape += [jax.ShapeDtypeStruct(m.shape, jnp.float32) for m in masters]
    out_shape += [
        jax.ShapeDtypeStruct((n, 2, w), jnp.float32),
        jax.ShapeDtypeStruct((2, w), jnp.float32),
    ]
    coded = [
        pltpu.VMEM((HALVES, groups, m.shape[0] // HALVES, m.shape[1]), jnp.bfloat16)
        for m in masters
    ]
    owns = [
        pltpu.VMEM((HALVES, m.shape[0] // HALVES, m.shape[1]), jnp.float32)
        for m in masters
    ]
    dma = pltpu.SemaphoreType.DMA
    vmem = pl.BlockSpec(memory_space=pltpu.VMEM)
    hbm = pl.BlockSpec(memory_space=pltpu.HBM)
    pin = lambda x: pltpu.with_memory_space_constraint(x, pltpu.HBM)
    outs = pl.pallas_call(
        functools.partial(kernel, n, kinds, limit),
        out_shape=[pltpu.VMEM(x.shape, x.dtype) for x in out_shape],
        in_specs=[hbm] * len(partials) + [vmem] * (len(partials) + 4),
        out_specs=[vmem] * len(out_shape),
        scratch_shapes=coded * 4
        + owns
        + [pltpu.VMEM(p.shape[1:], jnp.float32) for p in partials]
        + [pltpu.VMEM((n, 2, w), jnp.float32)] * 2
        + [dma((len(partials),))]
        + [dma((chunk_count,))] * 2
        + [dma((chunk_count, groups))] * 2
        + [dma((2, chunk_count, groups))]
        + [dma((chunk_count, groups))] * 3
        + [dma((n,))] * 4,
        compiler_params=pltpu.CompilerParams(collective_id=0, has_side_effects=True, vmem_limit_bytes=40 << 20),
    )(
        *(pin(x) for x in partials),
        *(pin(x) for x in masters),
        pin(partial_norm.reshape(n, 1, w)),
        pin(partial_bias.reshape(n, 1, w)),
        pin(master_norm.reshape(1, w)),
        pin(master_bias.reshape(1, w)),
    )
    large, (vec_all, vec_mine) = outs[:8], outs[8:]
    tail_shape = [jax.ShapeDtypeStruct(x.shape, x.dtype) for x in large]
    tail_shape += [jax.ShapeDtypeStruct((n, w), jnp.bfloat16)] * 2
    tail_shape += [jax.ShapeDtypeStruct((1, w), jnp.float32)] * 2
    outs = pl.pallas_call(
        functools.partial(hand_over, len(large)),
        out_shape=tail_shape,
        in_specs=[vmem] * (len(large) + 2),
        out_specs=[hbm] * len(large) + [vmem] * 4,
        scratch_shapes=[dma((len(large),))],
        compiler_params=pltpu.CompilerParams(vmem_limit_bytes=8 << 20),
    )(*(pltpu.with_memory_space_constraint(x, pltpu.VMEM) for x in (*large, vec_all, vec_mine)))
    computes, steppeds, vectors = outs[:4], outs[4:8], outs[8:]
    if not wide:
        computes = (*computes[:3], computes[3].T)
        steppeds = (*steppeds[:3], steppeds[3].T)
    norm, bias, norm_step, bias_step = (v.reshape(-1) for v in vectors)
    return (*computes, norm, bias, *steppeds, norm_step, bias_step)


def solution(mesh):
    in_specs = (
        P("batch", None, "cols"),
        P("batch", None, "cols"),
        P("batch", None, "cols"),
        P("batch", "cols", None),
        P("batch", None),
        P("batch", None),
        P("batch", "cols"),
        P("batch", "cols"),
        P("batch", "cols"),
        P("cols", "batch"),
        P("batch"),
        P("batch"),
    )
    out_specs = (
        P(None, "cols"),
        P(None, "cols"),
        P(None, "cols"),
        P("cols", None),
        P(),
        P(),
        P("batch", "cols"),
        P("batch", "cols"),
        P("batch", "cols"),
        P("cols", "batch"),
        P("batch"),
        P("batch"),
    )
    return jax.shard_map(
        per_device, mesh=mesh, in_specs=in_specs, out_specs=out_specs, check_vma=False
    )
```

```python
import functools

import jax
import jax.numpy as jnp
from jax import lax
from jax.experimental import pallas as pl
from jax.experimental.pallas import tpu as pltpu
from jax.sharding import PartitionSpec as P

learn_rate = 0.4
HALVES = 2
SPAN = 125.0

PLAN = (
    (0, 0, 4, "Z", "Z"),
    (0, 4, 4, "Z", "Z"),
    (1, 0, 4, "X", "X"),
    (1, 4, 4, "X", "X"),
    (2, 0, 4, "X", "X"),
    (2, 4, 4, "X", "X"),
    (3, 0, 4, "X", "X"),
    (3, 4, 4, "X", "X"),
)
ORDERS = (
    (
        "0:z0",
        "6:x1",
        "8:x1",
        "1:z0",
        "7:x1",
        "5:x1",
        "8:z0",
        "6:z0",
        "7:z0",
        "2:x1",
        "3:x1",
        "5:z0",
        "4:x1",
        "2:z0",
        "0:zf",
        "3:z0",
        "4:z0",
        "1:zf",
        "0:f",
        "6:f",
        "5:r1",
        "5:f",
        "1:f",
        "8:f",
        "2:f",
        "6:r1",
        "7:r1",
        "0:b0",
        "7:f",
        "6:r2",
        "1:b0",
        "7:r2",
        "3:f",
        "5:r2",
        "4:f",
        "4:r1",
        "3:r1",
        "2:r1",
        "8:r3",
        "6:r3",
        "8:r1",
        "4:r2",
        "2:r3",
        "3:r2",
        "2:r2",
        "5:r3",
        "3:r3",
        "7:r3",
        "8:r2",
        "4:r3",
    ),
    (
        "5:x1",
        "6:x1",
        "8:x1",
        "7:x1",
        "2:x1",
        "4:x1",
        "0:a",
        "1:a",
        "6:a",
        "3:x1",
        "0:b",
        "0:zf",
        "7:a",
        "8:a",
        "1:b",
        "5:a",
        "1:zf",
        "6:b",
        "6:f",
        "7:b",
        "2:a",
        "7:f",
        "0:f",
        "5:f",
        "5:b",
        "3:a",
        "8:b",
        "6:rM",
        "2:b",
        "0:b0",
        "8:f",
        "4:a",
        "7:rM",
        "5:rM",
        "2:f",
        "3:b",
        "3:f",
        "6:rE",
        "1:f",
        "4:b",
        "4:f",
        "1:rE",
        "8:rE",
        "2:rM",
        "5:rE",
        "6:rF",
        "3:rM",
        "2:rE",
        "1:b0",
        "0:sE",
        "0:rM",
        "3:rE",
        "8:rF",
        "4:rM",
        "2:rF",
        "0:sM",
        "5:rF",
        "7:rE",
        "4:rE",
        "1:sE",
        "1:rM",
        "3:rF",
        "8:rM",
        "7:rF",
        "0:rE",
        "4:rF",
        "0:sF",
        "1:sF",
        "1:rF",
        "0:rF",
        "1:sM",
    ),
)


def encode(x, limit):
    power = jnp.exp2(jnp.abs(x) * (2 * SPAN / limit) - SPAN)
    return jnp.where(x < 0, -power, power).astype(jnp.bfloat16)


def decode(code, limit):
    y = code.astype(jnp.float32)
    size = (jnp.log2(jnp.abs(y)) + SPAN) * (limit / (2 * SPAN))
    return jnp.where(y < 0, -size, size)


def kernel(n, kinds, limit, *refs):
    count = len(kinds)
    groups = n // 2
    refs = list(refs)

    def take(k):
        out = refs[:k]
        del refs[:k]
        return out

    source, master = take(count), take(count)
    norm, bias, norm_master, bias_master = take(4)
    gathered, stepped = take(count), take(count)
    vec_all, vec_mine = take(2)
    pair_out, pair_in, part_out, part_in = take(count), take(count), take(count), take(count)
    own, partial = take(count), take(count)
    vec_out, vec_in = take(2)
    (in_sem,) = take(1)
    a_send, a_recv, b_send, b_recv, c_send, c_recv, d_send, d_recv = take(8)
    v_send, v_recv, w_send, w_recv = take(4)

    rate = n ** (-0.5)
    b = lax.axis_index("batch")
    side = lax.rem(b, 2)
    g = b // 2
    partner = b + 1 - 2 * side

    def remote(src, dst, send, recv, to):
        return pltpu.make_async_remote_copy(
            src_ref=src,
            dst_ref=dst,
            send_sem=send,
            recv_sem=recv,
            device_id={"batch": to},
            device_id_type=pl.DeviceIdType.MESH,
        )

    chunks = [(a, h) for h in range(HALVES) for a in range(count)]

    def place(a, h, d):
        rows, cols = stepped[a].shape
        r = rows // HALVES
        if kinds[a] == "rows":
            return pl.ds(pl.multiple_of(d * rows + h * r, r), r), pl.ds(0, cols)
        return pl.ds(h * r, r), pl.ds(pl.multiple_of(d * cols, cols), cols)

    def load(a, h, d):
        rows, cols = place(a, h, d)
        return partial[a][rows, cols]

    def other(k):
        return lax.rem(g + k, groups)

    loads = [
        pltpu.make_async_copy(source[a].at[0], partial[a], in_sem.at[a])
        for a in range(count)
    ]
    for copy in loads:
        copy.start()

    barrier = pltpu.get_barrier_semaphore()
    for k in range(1, n):
        pl.semaphore_signal(
            barrier,
            inc=1,
            device_id={"batch": lax.rem(b + k, n)},
            device_id_type=pl.DeviceIdType.MESH,
        )

    def pair_encode(c):
        a, h = chunks[c]

        def body(k, carry):
            pair_out[a][h, k] = encode(load(a, h, 2 * k + 1 - side), limit)
            return carry

        lax.fori_loop(0, groups, body, 0)

    def pair_copy(c):
        a, h = chunks[c]
        return remote(
            pair_out[a].at[h], pair_in[a].at[h], a_send.at[c], a_recv.at[c], partner
        )

    def part_copy(c, src_slot, dst_slot, to):
        a, h = chunks[c]
        return remote(
            part_out[a].at[h, src_slot],
            part_in[a].at[h, dst_slot],
            b_send.at[c, src_slot],
            b_recv.at[c, dst_slot],
            2 * to + side,
        )

    def pair_finish(c):
        a, h = chunks[c]
        pair_copy(c).wait_recv()
        for k in range(1, groups):
            to = other(k)
            total = load(a, h, 2 * to + side) + decode(pair_in[a][h, to], limit)
            part_out[a][h, to] = encode(total, 2 * limit)
            part_copy(c, to, g, to).start()
        own[a][h] = load(a, h, b) + decode(pair_in[a][h, g], limit)

    def line_copy(c, owner, way, to=None):
        a, h = chunks[c]
        rows, cols = place(a, h, owner)
        block = gathered[a].at[rows, cols]
        return remote(
            block,
            block,
            c_send.at[(way + 1) // 2, c, owner // 2],
            c_recv.at[c, owner // 2],
            b + 2 * way if to is None else to,
        )

    def has_next(way):
        return g < groups - 1 if way > 0 else g > 0

    def has_source(way, k):
        return g - k >= 0 if way > 0 else g + k < groups

    def cross_copy(c, owner, recv_owner):
        a, h = chunks[c]
        rows, cols = place(a, h, owner)
        block = gathered[a].at[rows, cols]
        return remote(
            block, block, d_send.at[c, owner // 2], d_recv.at[c, recv_owner // 2], partner
        )

    def part_finish(c):
        a, h = chunks[c]
        r = stepped[a].shape[0] // HALVES
        total = own[a][h]
        for k in range(1, groups):
            source = other(k)
            part_copy(c, source, source, source).wait_recv()
            total = total + decode(part_in[a][h, source], 2 * limit)
        rows = pl.ds(h * r, r)
        new = master[a][rows, :] - learn_rate * (total * rate)
        stepped[a][rows, :] = new
        at_rows, at_cols = place(a, h, b)
        gathered[a][at_rows, at_cols] = new.astype(jnp.bfloat16)
        for way in (1, -1):

            @pl.when(has_next(way))
            def _():
                line_copy(c, b, way).start()

        cross_copy(c, b, b).start()

    def line_finish(c, k):
        for way in (1, -1):

            @pl.when(has_source(way, k))
            def _():
                owner = b - 2 * k * way
                line_copy(c, owner, way, owner).wait_recv()

                @pl.when(has_next(way))
                def _():
                    line_copy(c, owner, way).start()

                cross_copy(c, owner, owner).start()

    def vec_copy(k):
        to = lax.rem(b + k, n)
        return remote(vec_out.at[to], vec_in.at[b], v_send.at[to], v_recv.at[b], to)

    def vec_back(k):
        to = lax.rem(b + k, n)
        return remote(vec_all.at[b], vec_all.at[b], w_send.at[to], w_recv.at[b], to)

    loads[0].wait()
    pair_encode(0)
    pl.semaphore_wait(barrier, n - 1)
    pair_copy(0).start()
    for d in range(n):
        vec_out[d, 0:1, :] = norm[d]
        vec_out[d, 1:2, :] = bias[d]
    for k in range(1, n):
        vec_copy(k).start()
    for c in range(1, len(chunks)):
        if c < count:
            loads[c].wait()
        pair_encode(c)
        pair_copy(c).start()

    for t in range(len(chunks) + groups):
        if t < len(chunks):
            pair_finish(t)
        if 0 <= t - 1 < len(chunks):
            part_finish(t - 1)
        if t == 1:
            total = vec_out[b]
            for k in range(1, n):
                source = lax.rem(b + k, n)
                remote(
                    vec_out.at[source],
                    vec_in.at[source],
                    v_send.at[source],
                    v_recv.at[source],
                    source,
                ).wait_recv()
                total = total + vec_in[source]
            mean = total * rate
            vec_mine[0:1, :] = norm_master[...] - learn_rate * mean[0:1]
            vec_mine[1:2, :] = bias_master[...] - learn_rate * mean[1:2]
            vec_all[b] = vec_mine[...]
            for k in range(1, n):
                vec_back(k).start()
        for k in range(groups - 1, 0, -1):
            if 0 <= t - 1 - k < len(chunks):
                line_finish(t - 1 - k, k)

    for c in range(len(chunks)):
        for k in range(groups):
            owner = 2 * other(k) + 1 - side
            cross_copy(c, owner, owner).wait_recv()
    for k in range(1, n):
        source = lax.rem(b + k, n)
        remote(
            vec_all.at[source],
            vec_all.at[source],
            w_send.at[source],
            w_recv.at[source],
            source,
        ).wait_recv()
    for k in range(1, n):
        vec_copy(k).wait_send()
        vec_back(k).wait_send()
    for c in range(len(chunks)):
        pair_copy(c).wait_send()
        for k in range(1, groups):
            to = other(k)
            part_copy(c, to, g, to).wait_send()
        for k in range(groups):
            owner = 2 * other(k) + side
            cross_copy(c, owner, owner).wait_send()
        for way in (1, -1):

            @pl.when(has_next(way))
            def _():
                line_copy(c, b, way).wait_send()

            for k in range(1, groups):

                @pl.when(has_source(way, k) & has_next(way))
                def _():
                    line_copy(c, b - 2 * k * way, way).wait_send()


def ladder(n, kinds, limit, plan, orders, *refs):
    count = len(kinds)
    groups = n // 2
    tiny = len(plan) - 1
    refs = list(refs)

    def take(k):
        out = refs[:k]
        del refs[:k]
        return out

    source, master_in = take(count), take(count)
    norm, bias, norm_in, bias_in = take(4)
    gathered, stepped = take(count), take(count)
    vec_all, vec_mine = take(2)
    chunks = len(plan)
    x1_out, x1_in = take(chunks), take(chunks)
    z_out, far_in, near_in = take(chunks), take(chunks), take(chunks)
    x2_out, x2_in, own = take(chunks), take(chunks), take(chunks)
    partial, master = take(count), take(count)
    vec_part, norm_part, bias_part, norm_master, bias_master = take(5)
    in_sem, master_sem, small_sem = take(3)
    x1_send, x1_recv, x2_send, x2_recv = take(4)
    z_send, z_recv, g_send, g_recv = take(4)

    rate = n ** (-0.5)
    b = lax.axis_index("batch")
    side = lax.rem(b, 2)
    g = b // 2
    partner = b + 1 - 2 * side
    way = jnp.where(g < groups // 2, 1, -1)
    is_end = (g == 0) | (g == groups - 1)

    loads = [
        pltpu.make_async_copy(source[a].at[0], partial[a], in_sem.at[a])
        for a in range(count)
    ]
    masters = [
        pltpu.make_async_copy(master_in[a], master[a], master_sem.at[a])
        for a in range(count)
    ]
    smalls = [
        pltpu.make_async_copy(src, dst, small_sem.at[i])
        for i, (src, dst) in enumerate(
            (
                (norm, norm_part),
                (bias, bias_part),
                (norm_in, norm_master),
                (bias_in, bias_master),
            )
        )
    ]

    def remote(src, dst, send, recv, to):
        return pltpu.make_async_remote_copy(
            src_ref=src,
            dst_ref=dst,
            send_sem=send,
            recv_sem=recv,
            device_id={"batch": to},
            device_id_type=pl.DeviceIdType.MESH,
        )

    def place(c, d):
        a, start, size = plan[c][:3]
        rows, cols = stepped[a].shape
        if kinds[a] == "rows":
            return pl.ds(pl.multiple_of(d * rows + start, 16), size), pl.ds(0, cols)
        return pl.ds(start, size), pl.ds(pl.multiple_of(d * cols, cols), cols)

    def load(c, d):
        if c == tiny:
            return vec_part[d]
        rows, cols = place(c, d)
        return partial[plan[c][0]][rows, cols]

    def block(c, d):
        if c == tiny:
            return vec_all.at[d]
        rows, cols = place(c, d)
        return gathered[plan[c][0]].at[rows, cols]

    def pack(c, x, terms):
        return x if c == tiny else encode(x, terms * limit)

    def unpack(c, code, terms):
        return code if c == tiny else decode(code, terms * limit)

    def x1_copy(c):
        return remote(x1_out[c], x1_in[c], x1_send.at[c], x1_recv.at[c], partner)

    def x2_copy(c):
        return remote(x2_out[c], x2_in[c], x2_send.at[c], x2_recv.at[c], partner)

    def program(end, order):
        waited = set()
        sent = []
        met = []
        out_to = b + 2 * way
        near_to = b - 2 * way
        lines = ("out",) if end else ("near", "out")

        def first(key, wait):
            if key not in waited:
                waited.add(key)
                wait()

        def send(copy):
            if not met:
                met.append(True)
                pl.semaphore_wait(barrier, 2 if end else 3)
            copy.start()
            sent.append(copy)

        def need(c):
            if c < tiny:
                first(("load", plan[c][0]), loads[plan[c][0]].wait)
                return

            def gather():
                for copy in smalls:
                    copy.wait()
                for d in range(n):
                    vec_part[d, 0:1, :] = norm_part[d]
                    vec_part[d, 1:2, :] = bias_part[d]

            first("small", gather)

        def z_copy(c, kind):
            m = 2 if plan[c][3] == "Z" else 1
            if kind == "end":
                lo, size, slot, dst, to = 0, 3 * m, 0, far_in[c], out_to
            elif kind == "mid":
                dst = near_in[c].at[pl.ds(0, 2 * m)]
                lo, size, slot, to = 0, 2 * m, 0, out_to
            else:
                dst = near_in[c].at[pl.ds(0, m)]
                lo, size, slot, to = 2 * m, m, 1, near_to
            return remote(
                z_out[c].at[pl.ds(lo, size)],
                dst,
                z_send.at[slot, c],
                z_recv.at[0 if kind == "end" else 1, c],
                to,
            )

        def got_far(c):
            first(("far", c), z_copy(c, "end").wait_recv)

        def got_near(c):
            first(("near", c), z_copy(c, "back" if end else "mid").wait_recv)

        def got_x1(c):
            first(("x1", c), x1_copy(c).wait_recv)

        def pair(c, z):
            return load(c, 2 * z + side) + unpack(c, x1_in[c][z], 1)

        def each(lo, hi, fn):
            def body(j, carry):
                fn(j)
                return carry

            lax.fori_loop(lo, hi, body, 0)

        def x1(c):
            need(c)

            def put(z):
                x1_out[c][z] = pack(c, load(c, 2 * z + 1 - side), 1)

            each(0, groups, put)
            send(x1_copy(c))

        def z0(c):
            need(c)
            if plan[c][3] == "Z":

                def put(j):
                    d = 2 * (g + way * (j // 2 + 1)) + lax.rem(j, 2)
                    z_out[c][j] = pack(c, load(c, d), 1)

                each(0, 6, put)
            else:
                got_x1(c)

                def put(j):
                    z_out[c][j] = pack(c, pair(c, g + way * (j + 1)), 2)

                each(0, 3, put)
            send(z_copy(c, "end"))

        def a(c):
            need(c)
            if plan[c][3] == "Z":
                got_far(c)

                def put(j):
                    d = 2 * (g + way * (j // 2 + 1)) + lax.rem(j, 2)
                    total = load(c, d) + unpack(c, far_in[c][j + 2], 1)
                    z_out[c][j] = pack(c, total, 2)

                each(0, 4, put)
            else:
                got_x1(c)
                got_far(c)

                def put(j):
                    total = pair(c, g + way * (j + 1)) + unpack(c, far_in[c][j + 1], 2)
                    z_out[c][j] = pack(c, total, 4)

                each(0, 2, put)
            send(z_copy(c, "mid"))

        def back(c):
            need(c)
            z = g - way
            if plan[c][3] == "Z":
                got_near(c)

                def put(s):
                    total = load(c, 2 * z + s) + unpack(c, near_in[c][2 + s], 2)
                    z_out[c][4 + s] = pack(c, total, 3)

                each(0, 2, put)
            else:
                got_x1(c)
                got_near(c)
                total = pair(c, z) + unpack(c, near_in[c][1], 4)
                z_out[c][2] = pack(c, total, 6)
            send(z_copy(c, "back"))

        def line_sum(c, s):
            total = load(c, 2 * g + s)
            if end:
                return total + unpack(c, near_in[c][s], 3)
            return total + unpack(c, far_in[c][s], 1) + unpack(c, near_in[c][s], 2)

        def zf(c):
            need(c)
            got_near(c)
            if not end:
                got_far(c)
            x2_out[c][...] = pack(c, line_sum(c, 1 - side), 4)
            send(x2_copy(c))
            own[c][...] = line_sum(c, side)

        def block_copy(c, d, lane):
            to = {"x": partner, "out": out_to, "near": near_to}[lane]
            slot = {"x": 0, "out": 1, "near": 2}[lane]
            ref = block(c, d)
            return remote(ref, ref, g_send.at[slot, c, d], g_recv.at[c, d], to)

        def got(c, step, s):
            d = 2 * (g + way * step) + (1 - side if s else side)
            first(("block", c, step, s), block_copy(c, d, "x").wait_recv)
            return d

        def f(c):
            need(c)
            if plan[c][3] == "Z":
                x2_copy(c).wait_recv()
                total = own[c][...] + unpack(c, x2_in[c][...], 4)
            else:
                got_x1(c)
                got_near(c)
                total = pair(c, g)
                if end:
                    total = total + unpack(c, near_in[c][0], 6)
                else:
                    got_far(c)
                    total = total + unpack(c, far_in[c][0], 2)
                    total = total + unpack(c, near_in[c][0], 4)
            if c == tiny:
                mean = total * rate
                vec_mine[0:1, :] = norm_master[...] - learn_rate * mean[0:1]
                vec_mine[1:2, :] = bias_master[...] - learn_rate * mean[1:2]
                vec_all[b] = vec_mine[...]
            else:
                k, start, size = plan[c][:3]
                first(("master", k), masters[k].wait)
                rows = pl.ds(start, size)
                new = master[k][rows, :] - learn_rate * (total * rate)
                stepped[k][rows, :] = new
                at_rows, at_cols = place(c, b)
                gathered[k][at_rows, at_cols] = new.astype(jnp.bfloat16)
            for lane in lines + ("x",):
                send(block_copy(c, b, lane))

        def relay(step, s, lanes):
            def go(c):
                d = got(c, step, s)
                for lane in lanes if plan[c][4] == "Z" else lanes + ("x",):
                    send(block_copy(c, d, lane))

            return go

        moves = {"x1": x1, "z0": z0, "a": a, "b": back, "zf": zf, "f": f}
        moves["b0"] = relay(0, 1, lines)
        for step in (1, 2, 3):
            moves[f"r{step}"] = relay(step, 0, ())
        for name, step, lane in (("E", -1, "out"), ("M", 1, "near"), ("F", 2, "near")):
            moves["r" + name] = relay(step, 0, (lane,))
            moves["s" + name] = relay(step, 1, (lane,))

        for to in (partner, out_to) if end else (partner, out_to, near_to):
            pl.semaphore_signal(
                barrier,
                inc=1,
                device_id={"batch": to},
                device_id_type=pl.DeviceIdType.MESH,
            )
        for k in dict.fromkeys(plan[c][0] for c, _ in order if c < tiny):
            loads[k].start()
        for copy in smalls + masters:
            copy.start()
        for c, move in order:
            moves[move](c)
        for c in range(chunks):
            for step in (0, 1, 2, 3) if end else (-1, 0, 1, 2):
                for s in range(2):
                    if step or s:
                        got(c, step, s)
        for copy in sent:
            copy.wait_send()

    barrier = pltpu.get_barrier_semaphore()

    @pl.when(is_end)
    def _():
        program(True, orders[0])

    @pl.when(jnp.logical_not(is_end))
    def _():
        program(False, orders[1])


def hand_over(count, *refs):
    sources, vec_all, vec_mine = refs[:count], refs[count], refs[count + 1]
    targets = refs[count + 2 : 2 * count + 2]
    norm, bias, norm_step, bias_step = refs[2 * count + 2 : 2 * count + 6]
    (out_sem,) = refs[2 * count + 6 :]
    outs = [
        pltpu.make_async_copy(sources[i], targets[i], out_sem.at[i]) for i in range(count)
    ]
    for copy in outs:
        copy.start()
    norm[...] = vec_all[:, 0, :].astype(jnp.bfloat16)
    bias[...] = vec_all[:, 1, :].astype(jnp.bfloat16)
    norm_step[...] = vec_mine[0:1, :]
    bias_step[...] = vec_mine[1:2, :]
    for copy in outs:
        copy.wait()


def exchange_ladder(partials, masters, vectors, limit, kinds):
    n = lax.axis_size("batch")
    groups = n // 2
    w = vectors[-1].shape[1]
    plan = []
    for a, start, size, reduce_kind, gather_kind in PLAN:
        rows = masters[a].shape[0]
        plan.append((a, start * rows // 8, size * rows // 8, reduce_kind, gather_kind))
    shapes = [(size, masters[a].shape[1]) for a, _, size, _, _ in plan] + [(2, w)]
    types = [jnp.bfloat16] * len(plan) + [jnp.float32]
    plan.append((None, 0, 2, "X", "X"))
    orders = [
        [(int(c), move) for c, move in (step.split(":") for step in order)]
        for order in ORDERS
    ]

    def buffers(lead):
        return [pltpu.VMEM((*lead(p), *s), t) for p, s, t in zip(plan, shapes, types)]

    def line(k):
        return buffers(lambda p: (2 * k if p[3] == "Z" else k,))

    dma = pltpu.SemaphoreType.DMA
    chunks = len(plan)
    out_shape = [pltpu.VMEM(p.shape[1:], jnp.bfloat16) for p in partials]
    out_shape += [pltpu.VMEM(m.shape, jnp.float32) for m in masters]
    out_shape += [pltpu.VMEM((n, 2, w), jnp.float32), pltpu.VMEM((2, w), jnp.float32)]
    scratch = buffers(lambda p: (groups if p[3] == "X" else 1,)) * 2
    scratch += line(3) * 2 + line(2)
    scratch += buffers(lambda p: ()) * 2
    scratch += [pltpu.VMEM(s, jnp.float32) for s in shapes]
    scratch += [pltpu.VMEM(p.shape[1:], jnp.float32) for p in partials]
    scratch += [pltpu.VMEM(m.shape, jnp.float32) for m in masters]
    scratch += [pltpu.VMEM((n, 2, w), jnp.float32)]
    scratch += [pltpu.VMEM((n, 1, w), jnp.float32)] * 2
    scratch += [pltpu.VMEM((1, w), jnp.float32)] * 2
    scratch += [dma((len(partials),))] * 2 + [dma((4,))]
    scratch += [dma((chunks,))] * 4 + [dma((2, chunks))] * 2
    scratch += [dma((3, chunks, n)), dma((chunks, n))]
    args = (*partials, *masters, *vectors)
    return pl.pallas_call(
        functools.partial(ladder, n, kinds, limit, plan, orders),
        out_shape=out_shape,
        in_specs=[pl.BlockSpec(memory_space=pltpu.HBM)] * len(args),
        out_specs=[pl.BlockSpec(memory_space=pltpu.VMEM)] * len(out_shape),
        scratch_shapes=scratch,
        compiler_params=pltpu.CompilerParams(
            collective_id=0, has_side_effects=True, vmem_limit_bytes=40 << 20
        ),
    )(*(pltpu.with_memory_space_constraint(x, pltpu.HBM) for x in args))


def per_device(
    partial_query,
    partial_key,
    partial_value,
    partial_mixed,
    partial_norm,
    partial_bias,
    master_query,
    master_key,
    master_value,
    master_mixed,
    master_norm,
    master_bias,
):
    n = lax.axis_size("batch")
    groups = n // 2
    limit = 0.875 if n <= 8 else 1.25
    wide = master_mixed.shape[1] % 128 == 0
    kinds = ("rows", "rows", "rows", "cols" if wide else "rows")
    if not wide:
        partial_mixed = jnp.swapaxes(partial_mixed, 1, 2)
        master_mixed = master_mixed.T
    partials = (partial_query, partial_key, partial_value, partial_mixed)
    masters = (master_query, master_key, master_value, master_mixed)
    chunk_count = len(partials) * HALVES
    w = master_norm.shape[0]

    out_shape = [jax.ShapeDtypeStruct(p.shape[1:], jnp.bfloat16) for p in partials]
    out_shape += [jax.ShapeDtypeStruct(m.shape, jnp.float32) for m in masters]
    out_shape += [
        jax.ShapeDtypeStruct((n, 2, w), jnp.float32),
        jax.ShapeDtypeStruct((2, w), jnp.float32),
    ]
    coded = [
        pltpu.VMEM((HALVES, groups, m.shape[0] // HALVES, m.shape[1]), jnp.bfloat16)
        for m in masters
    ]
    owns = [
        pltpu.VMEM((HALVES, m.shape[0] // HALVES, m.shape[1]), jnp.float32)
        for m in masters
    ]
    dma = pltpu.SemaphoreType.DMA
    vmem = pl.BlockSpec(memory_space=pltpu.VMEM)
    hbm = pl.BlockSpec(memory_space=pltpu.HBM)
    pin = lambda x: pltpu.with_memory_space_constraint(x, pltpu.HBM)
    exchange = pl.pallas_call(
        functools.partial(kernel, n, kinds, limit),
        out_shape=[pltpu.VMEM(x.shape, x.dtype) for x in out_shape],
        in_specs=[hbm] * len(partials) + [vmem] * (len(partials) + 4),
        out_specs=[vmem] * len(out_shape),
        scratch_shapes=coded * 4
        + owns
        + [pltpu.VMEM(p.shape[1:], jnp.float32) for p in partials]
        + [pltpu.VMEM((n, 2, w), jnp.float32)] * 2
        + [dma((len(partials),))]
        + [dma((chunk_count,))] * 2
        + [dma((chunk_count, groups))] * 2
        + [dma((2, chunk_count, groups))]
        + [dma((chunk_count, groups))] * 3
        + [dma((n,))] * 4,
        compiler_params=pltpu.CompilerParams(collective_id=0, has_side_effects=True, vmem_limit_bytes=40 << 20),
    )
    vectors = (
        partial_norm.reshape(n, 1, w),
        partial_bias.reshape(n, 1, w),
        master_norm.reshape(1, w),
        master_bias.reshape(1, w),
    )
    if n == 8 and wide and all(m.shape[0] % 128 == 0 for m in masters):
        outs = exchange_ladder(partials, masters, vectors, limit, kinds)
    else:
        outs = exchange(*(pin(x) for x in (*partials, *masters, *vectors)))
    large, (vec_all, vec_mine) = outs[:8], outs[8:]
    tail_shape = [jax.ShapeDtypeStruct(x.shape, x.dtype) for x in large]
    tail_shape += [jax.ShapeDtypeStruct((n, w), jnp.bfloat16)] * 2
    tail_shape += [jax.ShapeDtypeStruct((1, w), jnp.float32)] * 2
    outs = pl.pallas_call(
        functools.partial(hand_over, len(large)),
        out_shape=tail_shape,
        in_specs=[vmem] * (len(large) + 2),
        out_specs=[hbm] * len(large) + [vmem] * 4,
        scratch_shapes=[dma((len(large),))],
        compiler_params=pltpu.CompilerParams(vmem_limit_bytes=8 << 20),
    )(*(pltpu.with_memory_space_constraint(x, pltpu.VMEM) for x in (*large, vec_all, vec_mine)))
    computes, steppeds, vectors = outs[:4], outs[4:8], outs[8:]
    if not wide:
        computes = (*computes[:3], computes[3].T)
        steppeds = (*steppeds[:3], steppeds[3].T)
    norm, bias, norm_step, bias_step = (v.reshape(-1) for v in vectors)
    return (*computes, norm, bias, *steppeds, norm_step, bias_step)


def solution(mesh):
    in_specs = (
        P("batch", None, "cols"),
        P("batch", None, "cols"),
        P("batch", None, "cols"),
        P("batch", "cols", None),
        P("batch", None),
        P("batch", None),
        P("batch", "cols"),
        P("batch", "cols"),
        P("batch", "cols"),
        P("cols", "batch"),
        P("batch"),
        P("batch"),
    )
    out_specs = (
        P(None, "cols"),
        P(None, "cols"),
        P(None, "cols"),
        P("cols", None),
        P(),
        P(),
        P("batch", "cols"),
        P("batch", "cols"),
        P("batch", "cols"),
        P("cols", "batch"),
        P("batch"),
        P("batch"),
    )
    return jax.shard_map(
        per_device, mesh=mesh, in_specs=in_specs, out_specs=out_specs, check_vma=False
    )
```

```python
import functools

import jax
import jax.numpy as jnp
from jax import lax
from jax.experimental import pallas as pl
from jax.experimental.pallas import tpu as pltpu
from jax.sharding import PartitionSpec as P

learn_rate = 0.4
HALVES = 2
SPAN = 125.0
PIECES = 2

PLAN = (
    (0, 0, 4, "Z", "Z"),
    (0, 4, 2, "Z", "Z"),
    (0, 6, 2, "X", "X"),
    (1, 0, 4, "X", "X"),
    (1, 4, 4, "X", "X"),
    (2, 0, 4, "X", "X"),
    (2, 4, 4, "X", "X"),
    (3, 0, 4, "X", "X"),
    (3, 4, 4, "X", "X"),
)
ORDERS = (
    (
        "9:x1",
        "4:x1",
        "1:z0",
        "7:x1",
        "2:x1",
        "5:x1",
        "0:z0",
        "8:x1",
        "6:x1",
        "4:z0",
        "7:z0",
        "2:z0",
        "3:x1",
        "9:z0",
        "5:z0",
        "1:zf",
        "8:z0",
        "6:z0",
        "4:f",
        "0:zf",
        "3:z0",
        "1:f",
        "7:f",
        "7:r1",
        "0:f",
        "2:f",
        "5:r1",
        "5:f",
        "4:r2",
        "2:r2",
        "2:r1",
        "4:r1",
        "9:f",
        "1:b0",
        "8:f",
        "7:r2",
        "5:r2",
        "8:r1",
        "6:f",
        "3:f",
        "9:r2",
        "6:r1",
        "0:b0",
        "8:r2",
        "6:r2",
        "3:r1",
        "5:r3",
        "2:r3",
        "4:r3",
        "9:r3",
        "9:r1",
        "7:r3",
        "8:r3",
        "6:r3",
        "3:r2",
        "3:r3",
    ),
    (
        "4:x1",
        "9:x1",
        "7:x1",
        "5:x1",
        "1:a",
        "1:zf",
        "0:a",
        "1:b",
        "2:x1",
        "8:x1",
        "6:x1",
        "4:a",
        "1:f",
        "7:a",
        "0:b",
        "2:a",
        "9:a",
        "0:zf",
        "4:f",
        "4:b",
        "1:rM",
        "3:x1",
        "5:a",
        "7:b",
        "2:f",
        "9:b",
        "2:b",
        "1:b0",
        "7:f",
        "4:rM",
        "8:a",
        "5:f",
        "5:b",
        "0:f",
        "1:sM",
        "2:rM",
        "6:a",
        "8:f",
        "8:b",
        "5:rM",
        "7:rM",
        "3:a",
        "6:b",
        "9:f",
        "6:f",
        "4:rE",
        "8:rM",
        "5:rE",
        "3:b",
        "9:rM",
        "2:rE",
        "9:rE",
        "3:f",
        "7:rE",
        "8:rE",
        "6:rM",
        "0:b0",
        "2:rF",
        "5:rF",
        "6:rE",
        "4:rF",
        "9:rF",
        "7:rF",
        "1:sE",
        "1:rE",
        "8:rF",
        "3:rE",
        "0:rE",
        "6:rF",
        "3:rM",
        "0:sE",
        "0:sM",
        "3:rF",
        "0:rF",
        "1:rF",
        "0:sF",
        "1:sF",
        "0:rM",
    ),
)


def encode(x, limit):
    power = jnp.exp2(jnp.abs(x) * (2 * SPAN / limit) - SPAN)
    return jnp.where(x < 0, -power, power).astype(jnp.bfloat16)


def decode(code, limit):
    y = code.astype(jnp.float32)
    size = (jnp.log2(jnp.abs(y)) + SPAN) * (limit / (2 * SPAN))
    return jnp.where(y < 0, -size, size)


def kernel(n, kinds, limit, *refs):
    count = len(kinds)
    groups = n // 2
    refs = list(refs)

    def take(k):
        out = refs[:k]
        del refs[:k]
        return out

    source, master = take(count), take(count)
    norm, bias, norm_master, bias_master = take(4)
    gathered, stepped = take(count), take(count)
    vec_all, vec_mine = take(2)
    pair_out, pair_in, part_out, part_in = take(count), take(count), take(count), take(count)
    own, partial = take(count), take(count)
    vec_out, vec_in = take(2)
    (in_sem,) = take(1)
    a_send, a_recv, b_send, b_recv, c_send, c_recv, d_send, d_recv = take(8)
    v_send, v_recv, w_send, w_recv = take(4)

    rate = n ** (-0.5)
    b = lax.axis_index("batch")
    side = lax.rem(b, 2)
    g = b // 2
    partner = b + 1 - 2 * side

    def remote(src, dst, send, recv, to):
        return pltpu.make_async_remote_copy(
            src_ref=src,
            dst_ref=dst,
            send_sem=send,
            recv_sem=recv,
            device_id={"batch": to},
            device_id_type=pl.DeviceIdType.MESH,
        )

    chunks = [(a, h) for h in range(HALVES) for a in range(count)]

    def place(a, h, d):
        rows, cols = stepped[a].shape
        r = rows // HALVES
        if kinds[a] == "rows":
            return pl.ds(pl.multiple_of(d * rows + h * r, r), r), pl.ds(0, cols)
        return pl.ds(h * r, r), pl.ds(pl.multiple_of(d * cols, cols), cols)

    def load(a, h, d):
        rows, cols = place(a, h, d)
        return partial[a][rows, cols]

    def other(k):
        return lax.rem(g + k, groups)

    loads = [
        pltpu.make_async_copy(source[a].at[0], partial[a], in_sem.at[a])
        for a in range(count)
    ]
    for copy in loads:
        copy.start()

    barrier = pltpu.get_barrier_semaphore()
    for k in range(1, n):
        pl.semaphore_signal(
            barrier,
            inc=1,
            device_id={"batch": lax.rem(b + k, n)},
            device_id_type=pl.DeviceIdType.MESH,
        )

    def pair_encode(c):
        a, h = chunks[c]

        def body(k, carry):
            pair_out[a][h, k] = encode(load(a, h, 2 * k + 1 - side), limit)
            return carry

        lax.fori_loop(0, groups, body, 0)

    def pair_copy(c):
        a, h = chunks[c]
        return remote(
            pair_out[a].at[h], pair_in[a].at[h], a_send.at[c], a_recv.at[c], partner
        )

    def part_copy(c, src_slot, dst_slot, to):
        a, h = chunks[c]
        return remote(
            part_out[a].at[h, src_slot],
            part_in[a].at[h, dst_slot],
            b_send.at[c, src_slot],
            b_recv.at[c, dst_slot],
            2 * to + side,
        )

    def pair_finish(c):
        a, h = chunks[c]
        pair_copy(c).wait_recv()
        for k in range(1, groups):
            to = other(k)
            total = load(a, h, 2 * to + side) + decode(pair_in[a][h, to], limit)
            part_out[a][h, to] = encode(total, 2 * limit)
            part_copy(c, to, g, to).start()
        own[a][h] = load(a, h, b) + decode(pair_in[a][h, g], limit)

    def line_copy(c, owner, way, to=None):
        a, h = chunks[c]
        rows, cols = place(a, h, owner)
        block = gathered[a].at[rows, cols]
        return remote(
            block,
            block,
            c_send.at[(way + 1) // 2, c, owner // 2],
            c_recv.at[c, owner // 2],
            b + 2 * way if to is None else to,
        )

    def has_next(way):
        return g < groups - 1 if way > 0 else g > 0

    def has_source(way, k):
        return g - k >= 0 if way > 0 else g + k < groups

    def cross_copy(c, owner, recv_owner):
        a, h = chunks[c]
        rows, cols = place(a, h, owner)
        block = gathered[a].at[rows, cols]
        return remote(
            block, block, d_send.at[c, owner // 2], d_recv.at[c, recv_owner // 2], partner
        )

    def part_finish(c):
        a, h = chunks[c]
        r = stepped[a].shape[0] // HALVES
        total = own[a][h]
        for k in range(1, groups):
            source = other(k)
            part_copy(c, source, source, source).wait_recv()
            total = total + decode(part_in[a][h, source], 2 * limit)
        rows = pl.ds(h * r, r)
        new = master[a][rows, :] - learn_rate * (total * rate)
        stepped[a][rows, :] = new
        at_rows, at_cols = place(a, h, b)
        gathered[a][at_rows, at_cols] = new.astype(jnp.bfloat16)
        for way in (1, -1):

            @pl.when(has_next(way))
            def _():
                line_copy(c, b, way).start()

        cross_copy(c, b, b).start()

    def line_finish(c, k):
        for way in (1, -1):

            @pl.when(has_source(way, k))
            def _():
                owner = b - 2 * k * way
                line_copy(c, owner, way, owner).wait_recv()

                @pl.when(has_next(way))
                def _():
                    line_copy(c, owner, way).start()

                cross_copy(c, owner, owner).start()

    def vec_copy(k):
        to = lax.rem(b + k, n)
        return remote(vec_out.at[to], vec_in.at[b], v_send.at[to], v_recv.at[b], to)

    def vec_back(k):
        to = lax.rem(b + k, n)
        return remote(vec_all.at[b], vec_all.at[b], w_send.at[to], w_recv.at[b], to)

    loads[0].wait()
    pair_encode(0)
    pl.semaphore_wait(barrier, n - 1)
    pair_copy(0).start()
    for d in range(n):
        vec_out[d, 0:1, :] = norm[d]
        vec_out[d, 1:2, :] = bias[d]
    for k in range(1, n):
        vec_copy(k).start()
    for c in range(1, len(chunks)):
        if c < count:
            loads[c].wait()
        pair_encode(c)
        pair_copy(c).start()

    for t in range(len(chunks) + groups):
        if t < len(chunks):
            pair_finish(t)
        if 0 <= t - 1 < len(chunks):
            part_finish(t - 1)
        if t == 1:
            total = vec_out[b]
            for k in range(1, n):
                source = lax.rem(b + k, n)
                remote(
                    vec_out.at[source],
                    vec_in.at[source],
                    v_send.at[source],
                    v_recv.at[source],
                    source,
                ).wait_recv()
                total = total + vec_in[source]
            mean = total * rate
            vec_mine[0:1, :] = norm_master[...] - learn_rate * mean[0:1]
            vec_mine[1:2, :] = bias_master[...] - learn_rate * mean[1:2]
            vec_all[b] = vec_mine[...]
            for k in range(1, n):
                vec_back(k).start()
        for k in range(groups - 1, 0, -1):
            if 0 <= t - 1 - k < len(chunks):
                line_finish(t - 1 - k, k)

    for c in range(len(chunks)):
        for k in range(groups):
            owner = 2 * other(k) + 1 - side
            cross_copy(c, owner, owner).wait_recv()
    for k in range(1, n):
        source = lax.rem(b + k, n)
        remote(
            vec_all.at[source],
            vec_all.at[source],
            w_send.at[source],
            w_recv.at[source],
            source,
        ).wait_recv()
    for k in range(1, n):
        vec_copy(k).wait_send()
        vec_back(k).wait_send()
    for c in range(len(chunks)):
        pair_copy(c).wait_send()
        for k in range(1, groups):
            to = other(k)
            part_copy(c, to, g, to).wait_send()
        for k in range(groups):
            owner = 2 * other(k) + side
            cross_copy(c, owner, owner).wait_send()
        for way in (1, -1):

            @pl.when(has_next(way))
            def _():
                line_copy(c, b, way).wait_send()

            for k in range(1, groups):

                @pl.when(has_source(way, k) & has_next(way))
                def _():
                    line_copy(c, b - 2 * k * way, way).wait_send()


def ladder(n, kinds, limit, plan, orders, *refs):
    count = len(kinds)
    groups = n // 2
    tiny = len(plan) - 1
    refs = list(refs)

    def take(k):
        out = refs[:k]
        del refs[:k]
        return out

    source, master_in = take(count), take(count)
    norm, bias, norm_in, bias_in = take(4)
    gathered, stepped = take(count), take(count)
    norm_out, bias_out, norm_step, bias_step = take(4)
    chunks = len(plan)
    x1_out, x1_in = take(chunks), take(chunks)
    z_out, far_in, near_in = take(chunks), take(chunks), take(chunks)
    x2_out, x2_in, own = take(chunks), take(chunks), take(chunks)
    partial, master = take(count), take(count)
    vec_all, vec_part, norm_part, bias_part, norm_master, bias_master = take(6)
    in_sem, master_sem, small_sem = take(3)
    out_sem, x1_recv, x2_recv, z_recv, g_recv = take(5)

    rate = n ** (-0.5)
    b = lax.axis_index("batch")
    side = lax.rem(b, 2)
    g = b // 2
    partner = b + 1 - 2 * side
    way = jnp.where(g < groups // 2, 1, -1)
    is_end = (g == 0) | (g == groups - 1)

    loads = [
        pltpu.make_async_copy(source[a].at[0], partial[a], in_sem.at[a])
        for a in range(count)
    ]
    masters = [
        pltpu.make_async_copy(master_in[a], master[a], master_sem.at[a])
        for a in range(count)
    ]
    smalls = [
        pltpu.make_async_copy(src, dst, small_sem.at[i])
        for i, (src, dst) in enumerate(
            (
                (norm, norm_part),
                (bias, bias_part),
                (norm_in, norm_master),
                (bias_in, bias_master),
            )
        )
    ]

    def remote(src, dst, send, recv, to):
        return pltpu.make_async_remote_copy(
            src_ref=src,
            dst_ref=dst,
            send_sem=send,
            recv_sem=recv,
            device_id={"batch": to},
            device_id_type=pl.DeviceIdType.MESH,
        )

    def place(c, d):
        a, start, size = plan[c][:3]
        rows, cols = stepped[a].shape
        if kinds[a] == "rows":
            return pl.ds(pl.multiple_of(d * rows + start, 16), size), pl.ds(0, cols)
        return pl.ds(start, size), pl.ds(pl.multiple_of(d * cols, cols), cols)

    def load(c, d):
        if c == tiny:
            return vec_part[d]
        rows, cols = place(c, d)
        return partial[plan[c][0]][rows, cols]

    def block(c, d):
        if c == tiny:
            return vec_all.at[d]
        rows, cols = place(c, d)
        return gathered[plan[c][0]].at[rows, cols]

    def pack(c, x, terms):
        return x if c == tiny else encode(x, terms * limit)

    def unpack(c, code, terms):
        return code if c == tiny else decode(code, terms * limit)

    def program(end, order):
        waited = set()
        sent = []
        out_to = b + 2 * way
        near_to = b - 2 * way
        lines = ("out",) if end else ("near", "out")

        def first(key, wait):
            if key not in waited:
                waited.add(key)
                wait()

        def slot():
            return out_sem.at[len(sent)]

        def send(copy):
            if not sent:
                pl.semaphore_wait(barrier, 2 if end else 3)
            copy.start()
            sent.append(copy)

        def x1_copy(c):
            return remote(x1_out[c], x1_in[c], slot(), x1_recv.at[c], partner)

        def x2_copy(c):
            return remote(x2_out[c], x2_in[c], slot(), x2_recv.at[c], partner)

        def need(c):
            if c < tiny:
                first(("load", plan[c][0]), loads[plan[c][0]].wait)
                return

            def gather():
                for copy in smalls:
                    copy.wait()
                for d in range(n):
                    vec_part[d, 0:1, :] = norm_part[d]
                    vec_part[d, 1:2, :] = bias_part[d]

            first("small", gather)

        def z_copy(c, kind):
            m = 2 if plan[c][3] == "Z" else 1
            if kind == "end":
                lo, size, dst, to = 0, 3 * m, far_in[c], out_to
            elif kind == "mid":
                dst = near_in[c].at[pl.ds(0, 2 * m)]
                lo, size, to = 0, 2 * m, out_to
            else:
                dst = near_in[c].at[pl.ds(0, m)]
                lo, size, to = 2 * m, m, near_to
            return remote(
                z_out[c].at[pl.ds(lo, size)],
                dst,
                slot(),
                z_recv.at[0 if kind == "end" else 1, c],
                to,
            )

        def got_far(c):
            first(("far", c), z_copy(c, "end").wait_recv)

        def got_near(c):
            first(("near", c), z_copy(c, "back" if end else "mid").wait_recv)

        def got_x1(c):
            first(("x1", c), x1_copy(c).wait_recv)

        def pair(c, z):
            return load(c, 2 * z + side) + unpack(c, x1_in[c][z], 1)

        def each(lo, hi, fn):
            def body(j, carry):
                fn(j)
                return carry

            lax.fori_loop(lo, hi, body, 0)

        def x1(c):
            need(c)

            def put(z):
                x1_out[c][z] = pack(c, load(c, 2 * z + 1 - side), 1)

            each(0, groups, put)
            send(x1_copy(c))

        def z0(c):
            need(c)
            if plan[c][3] == "Z":

                def put(j):
                    d = 2 * (g + way * (j // 2 + 1)) + lax.rem(j, 2)
                    z_out[c][j] = pack(c, load(c, d), 1)

                each(0, 6, put)
            else:
                got_x1(c)

                def put(j):
                    z_out[c][j] = pack(c, pair(c, g + way * (j + 1)), 2)

                each(0, 3, put)
            send(z_copy(c, "end"))

        def a(c):
            need(c)
            if plan[c][3] == "Z":
                got_far(c)

                def put(j):
                    d = 2 * (g + way * (j // 2 + 1)) + lax.rem(j, 2)
                    total = load(c, d) + unpack(c, far_in[c][j + 2], 1)
                    z_out[c][j] = pack(c, total, 2)

                each(0, 4, put)
            else:
                got_x1(c)
                got_far(c)

                def put(j):
                    total = pair(c, g + way * (j + 1)) + unpack(c, far_in[c][j + 1], 2)
                    z_out[c][j] = pack(c, total, 4)

                each(0, 2, put)
            send(z_copy(c, "mid"))

        def back(c):
            need(c)
            z = g - way
            if plan[c][3] == "Z":
                got_near(c)

                def put(s):
                    total = load(c, 2 * z + s) + unpack(c, near_in[c][2 + s], 2)
                    z_out[c][4 + s] = pack(c, total, 3)

                each(0, 2, put)
            else:
                got_x1(c)
                got_near(c)
                total = pair(c, z) + unpack(c, near_in[c][1], 4)
                z_out[c][2] = pack(c, total, 6)
            send(z_copy(c, "back"))

        def line_sum(c, s):
            total = load(c, 2 * g + s)
            if end:
                return total + unpack(c, near_in[c][s], 3)
            return total + unpack(c, far_in[c][s], 1) + unpack(c, near_in[c][s], 2)

        def zf(c):
            need(c)
            got_near(c)
            if not end:
                got_far(c)
            x2_out[c][...] = pack(c, line_sum(c, 1 - side), 4)
            send(x2_copy(c))
            own[c][...] = line_sum(c, side)

        def block_copy(c, d, lane):
            to = {
                "x": partner,
                "out": out_to,
                "near": near_to,
                "two": b + 4 * way,
                "three": b + 6 * way,
            }[lane]
            ref = block(c, d)
            return remote(ref, ref, slot(), g_recv.at[c, d], to)

        def got(c, step, s):
            d = 2 * (g + way * step) + (1 - side if s else side)
            first(("block", c, step, s), block_copy(c, d, "x").wait_recv)
            return d

        def f(c):
            need(c)
            if plan[c][3] == "Z":
                x2_copy(c).wait_recv()
                total = own[c][...] + unpack(c, x2_in[c][...], 4)
            else:
                got_x1(c)
                got_near(c)
                total = pair(c, g)
                if end:
                    total = total + unpack(c, near_in[c][0], 6)
                else:
                    got_far(c)
                    total = total + unpack(c, far_in[c][0], 2)
                    total = total + unpack(c, near_in[c][0], 4)
            if c == tiny:
                mean = total * rate
                norm_step[...] = norm_master[...] - learn_rate * mean[0:1]
                bias_step[...] = bias_master[...] - learn_rate * mean[1:2]
                vec_all[b, 0:1, :] = norm_step[...]
                vec_all[b, 1:2, :] = bias_step[...]
            else:
                k, start, size = plan[c][:3]
                first(("master", k), masters[k].wait)
                rows = pl.ds(start, size)
                new = master[k][rows, :] - learn_rate * (total * rate)
                stepped[k][rows, :] = new
                at_rows, at_cols = place(c, b)
                gathered[k][at_rows, at_cols] = new.astype(jnp.bfloat16)
            direct = ("three", "two") if end else ("two",)
            for lane in (direct if plan[c][4] == "D" else ()) + lines + ("x",):
                send(block_copy(c, b, lane))

        def relay(step, s, lanes):
            def go(c):
                d = got(c, step, s)
                kind = plan[c][4]
                lanes_now = (() if kind == "D" else lanes) + (() if kind == "Z" else ("x",))
                for lane in lanes_now:
                    send(block_copy(c, d, lane))

            return go

        moves = {"x1": x1, "z0": z0, "a": a, "b": back, "zf": zf, "f": f}
        moves["b0"] = relay(0, 1, lines)
        for step in (1, 2, 3):
            moves[f"r{step}"] = relay(step, 0, ())
        for name, step, lane in (("E", -1, "out"), ("M", 1, "near"), ("F", 2, "near")):
            moves["r" + name] = relay(step, 0, (lane,))
            moves["s" + name] = relay(step, 1, (lane,))

        for to in (partner, out_to) if end else (partner, out_to, near_to):
            pl.semaphore_signal(
                barrier,
                inc=1,
                device_id={"batch": to},
                device_id_type=pl.DeviceIdType.MESH,
            )
        for k in dict.fromkeys(plan[c][0] for c, _ in order if c < tiny):
            loads[k].start()
        for copy in smalls + masters:
            copy.start()
        for c, move in order:
            moves[move](c)
        steps = (0, 1, 2, 3) if end else (-1, 0, 1, 2)
        left = [(c, k, s) for c in range(chunks) for k in steps for s in (0, 1) if k or s]
        left.sort(key=lambda x: (x[0] != tiny, when(end, *x)))
        for c, step, s in left:
            if c == tiny:
                got(c, step, s)
        norm_out[...] = vec_all[:, 0, :].astype(jnp.bfloat16)
        bias_out[...] = vec_all[:, 1, :].astype(jnp.bfloat16)
        for copy in sent:
            copy.wait_send()
        for c, step, s in left:
            got(c, step, s)

    def when(end, c, step, s):
        own_side = {-1: "rE", 0: "f", 1: "r1" if end else "rM", 2: "r2" if end else "rF", 3: "r3"}
        if plan[c][4] != "Z" and s:
            moves, name = orders[0 if end else 1], own_side[step]
        else:
            names = {1: ("f", "b0"), 2: ("rM", "sM"), 3: ("rF", "sF")}
            moves, name = orders[1], names.get(step, ("f", "f"))[s]
        return moves.index((c, name)) / len(moves) if (c, name) in moves else 0

    barrier = pltpu.get_barrier_semaphore()

    @pl.when(is_end)
    def _():
        program(True, orders[0])

    @pl.when(jnp.logical_not(is_end))
    def _():
        program(False, orders[1])


def hand_over(count, *refs):
    sources, vec_all, vec_mine = refs[:count], refs[count], refs[count + 1]
    targets = refs[count + 2 : 2 * count + 2]
    norm, bias, norm_step, bias_step = refs[2 * count + 2 : 2 * count + 6]
    (out_sem,) = refs[2 * count + 6 :]
    outs = [
        pltpu.make_async_copy(sources[i], targets[i], out_sem.at[i]) for i in range(count)
    ]
    for copy in outs:
        copy.start()
    norm[...] = vec_all[:, 0, :].astype(jnp.bfloat16)
    bias[...] = vec_all[:, 1, :].astype(jnp.bfloat16)
    norm_step[...] = vec_mine[0:1, :]
    bias_step[...] = vec_mine[1:2, :]
    for copy in outs:
        copy.wait()


def deliver(count, *refs):
    sources, targets, sem = refs[:count], refs[count:-1], refs[-1]
    copies = []
    for i in range(count):
        rows = sources[i].shape[0]
        pieces = PIECES if rows >= 128 else 1
        for k in range(pieces):
            at = pl.ds(k * (rows // pieces), rows // pieces)
            copies.append(
                pltpu.make_async_copy(sources[i].at[at], targets[i].at[at], sem.at[i, k])
            )
    for copy in copies:
        copy.start()
    for copy in copies:
        copy.wait()


def exchange_ladder(partials, masters, vectors, limit, kinds):
    n = lax.axis_size("batch")
    groups = n // 2
    w = vectors[-1].shape[1]
    plan = []
    for a, start, size, reduce_kind, gather_kind in PLAN:
        rows = masters[a].shape[0]
        plan.append((a, start * rows // 8, size * rows // 8, reduce_kind, gather_kind))
    shapes = [(size, masters[a].shape[1]) for a, _, size, _, _ in plan] + [(2, w)]
    types = [jnp.bfloat16] * len(plan) + [jnp.float32]
    plan.append((None, 0, 2, "X", "X"))
    orders = [
        [(int(c), move) for c, move in (step.split(":") for step in order)]
        for order in ORDERS
    ]

    def buffers(lead):
        return [pltpu.VMEM((*lead(p), *s), t) for p, s, t in zip(plan, shapes, types)]

    def line(k):
        return buffers(lambda p: (2 * k if p[3] == "Z" else k,))

    dma = pltpu.SemaphoreType.DMA
    chunks = len(plan)
    out_shape = [pltpu.VMEM(p.shape[1:], jnp.bfloat16) for p in partials]
    out_shape += [pltpu.VMEM(m.shape, jnp.float32) for m in masters]
    out_shape += [pltpu.VMEM((n, w), jnp.bfloat16)] * 2
    out_shape += [pltpu.VMEM((1, w), jnp.float32)] * 2
    scratch = buffers(lambda p: (groups if p[3] == "X" else 1,)) * 2
    scratch += line(3) * 2 + line(2)
    scratch += buffers(lambda p: ()) * 2
    scratch += [pltpu.VMEM(s, jnp.float32) for s in shapes]
    scratch += [pltpu.VMEM(p.shape[1:], jnp.float32) for p in partials]
    scratch += [pltpu.VMEM(m.shape, jnp.float32) for m in masters]
    scratch += [pltpu.VMEM((n, 2, w), jnp.float32)] * 2
    scratch += [pltpu.VMEM((n, 1, w), jnp.float32)] * 2
    scratch += [pltpu.VMEM((1, w), jnp.float32)] * 2
    scratch += [dma((len(partials),))] * 2 + [dma((4,))]
    sends = sum(3 + {"X": 9, "Z": 11, "D": 7}[p[4]] for p in plan)
    scratch += [dma((sends,)), dma((chunks,)), dma((chunks,))]
    scratch += [dma((2, chunks)), dma((chunks, n))]
    args = (*partials, *masters, *vectors)
    outs = pl.pallas_call(
        functools.partial(ladder, n, kinds, limit, plan, orders),
        out_shape=out_shape,
        in_specs=[pl.BlockSpec(memory_space=pltpu.HBM)] * len(args),
        out_specs=[pl.BlockSpec(memory_space=pltpu.VMEM)] * len(out_shape),
        scratch_shapes=scratch,
        compiler_params=pltpu.CompilerParams(
            collective_id=0, has_side_effects=True, vmem_limit_bytes=40 << 20
        ),
    )(*(pltpu.with_memory_space_constraint(x, pltpu.HBM) for x in args))
    return pl.pallas_call(
        functools.partial(deliver, len(outs)),
        out_shape=[jax.ShapeDtypeStruct(x.shape, x.dtype) for x in outs],
        in_specs=[pl.BlockSpec(memory_space=pltpu.VMEM)] * len(outs),
        out_specs=[pl.BlockSpec(memory_space=pltpu.HBM)] * len(outs),
        scratch_shapes=[dma((len(outs), PIECES))],
        compiler_params=pltpu.CompilerParams(vmem_limit_bytes=8 << 20),
    )(*(pltpu.with_memory_space_constraint(x, pltpu.VMEM) for x in outs))


def per_device(
    partial_query,
    partial_key,
    partial_value,
    partial_mixed,
    partial_norm,
    partial_bias,
    master_query,
    master_key,
    master_value,
    master_mixed,
    master_norm,
    master_bias,
):
    n = lax.axis_size("batch")
    groups = n // 2
    limit = 0.875 if n <= 8 else 1.25
    wide = master_mixed.shape[1] % 128 == 0
    kinds = ("rows", "rows", "rows", "cols" if wide else "rows")
    if not wide:
        partial_mixed = jnp.swapaxes(partial_mixed, 1, 2)
        master_mixed = master_mixed.T
    partials = (partial_query, partial_key, partial_value, partial_mixed)
    masters = (master_query, master_key, master_value, master_mixed)
    chunk_count = len(partials) * HALVES
    w = master_norm.shape[0]

    out_shape = [jax.ShapeDtypeStruct(p.shape[1:], jnp.bfloat16) for p in partials]
    out_shape += [jax.ShapeDtypeStruct(m.shape, jnp.float32) for m in masters]
    out_shape += [
        jax.ShapeDtypeStruct((n, 2, w), jnp.float32),
        jax.ShapeDtypeStruct((2, w), jnp.float32),
    ]
    coded = [
        pltpu.VMEM((HALVES, groups, m.shape[0] // HALVES, m.shape[1]), jnp.bfloat16)
        for m in masters
    ]
    owns = [
        pltpu.VMEM((HALVES, m.shape[0] // HALVES, m.shape[1]), jnp.float32)
        for m in masters
    ]
    dma = pltpu.SemaphoreType.DMA
    vmem = pl.BlockSpec(memory_space=pltpu.VMEM)
    hbm = pl.BlockSpec(memory_space=pltpu.HBM)
    pin = lambda x: pltpu.with_memory_space_constraint(x, pltpu.HBM)
    exchange = pl.pallas_call(
        functools.partial(kernel, n, kinds, limit),
        out_shape=[pltpu.VMEM(x.shape, x.dtype) for x in out_shape],
        in_specs=[hbm] * len(partials) + [vmem] * (len(partials) + 4),
        out_specs=[vmem] * len(out_shape),
        scratch_shapes=coded * 4
        + owns
        + [pltpu.VMEM(p.shape[1:], jnp.float32) for p in partials]
        + [pltpu.VMEM((n, 2, w), jnp.float32)] * 2
        + [dma((len(partials),))]
        + [dma((chunk_count,))] * 2
        + [dma((chunk_count, groups))] * 2
        + [dma((2, chunk_count, groups))]
        + [dma((chunk_count, groups))] * 3
        + [dma((n,))] * 4,
        compiler_params=pltpu.CompilerParams(collective_id=0, has_side_effects=True, vmem_limit_bytes=40 << 20),
    )
    vectors = (
        partial_norm.reshape(n, 1, w),
        partial_bias.reshape(n, 1, w),
        master_norm.reshape(1, w),
        master_bias.reshape(1, w),
    )
    if n == 8 and wide and all(m.shape[0] % 128 == 0 for m in masters):
        outs = exchange_ladder(partials, masters, vectors, limit, kinds)
    else:
        outs = exchange(*(pin(x) for x in (*partials, *masters, *vectors)))
        large, (vec_all, vec_mine) = outs[:8], outs[8:]
        tail_shape = [jax.ShapeDtypeStruct(x.shape, x.dtype) for x in large]
        tail_shape += [jax.ShapeDtypeStruct((n, w), jnp.bfloat16)] * 2
        tail_shape += [jax.ShapeDtypeStruct((1, w), jnp.float32)] * 2
        outs = pl.pallas_call(
            functools.partial(hand_over, len(large)),
            out_shape=tail_shape,
            in_specs=[vmem] * (len(large) + 2),
            out_specs=[hbm] * len(large) + [vmem] * 4,
            scratch_shapes=[dma((len(large),))],
            compiler_params=pltpu.CompilerParams(vmem_limit_bytes=8 << 20),
        )(*(pltpu.with_memory_space_constraint(x, pltpu.VMEM) for x in (*large, vec_all, vec_mine)))
    computes, steppeds, vectors = outs[:4], outs[4:8], outs[8:]
    if not wide:
        computes = (*computes[:3], computes[3].T)
        steppeds = (*steppeds[:3], steppeds[3].T)
    norm, bias, norm_step, bias_step = (v.reshape(-1) for v in vectors)
    return (*computes, norm, bias, *steppeds, norm_step, bias_step)


def solution(mesh):
    in_specs = (
        P("batch", None, "cols"),
        P("batch", None, "cols"),
        P("batch", None, "cols"),
        P("batch", "cols", None),
        P("batch", None),
        P("batch", None),
        P("batch", "cols"),
        P("batch", "cols"),
        P("batch", "cols"),
        P("cols", "batch"),
        P("batch"),
        P("batch"),
    )
    out_specs = (
        P(None, "cols"),
        P(None, "cols"),
        P(None, "cols"),
        P("cols", None),
        P(),
        P(),
        P("batch", "cols"),
        P("batch", "cols"),
        P("batch", "cols"),
        P("cols", "batch"),
        P("batch"),
        P("batch"),
    )
    return jax.shard_map(
        per_device, mesh=mesh, in_specs=in_specs, out_specs=out_specs, check_vma=False
    )
```

```python
import functools
import math

import jax
import jax.numpy as jnp
from jax import lax
from jax.experimental import pallas as pl
from jax.experimental.pallas import tpu as pltpu
from jax.sharding import PartitionSpec as P

learn_rate = 0.4
HALVES = 2
SPAN = 125.0
PIECES = 2

PLAN = (
    (0, 0, 4, "Z", "Z"),
    (0, 4, 2, "Z", "Z"),
    (0, 6, 2, "X", "X"),
    (1, 0, 4, "X", "X"),
    (1, 4, 4, "X", "X"),
    (2, 0, 4, "X", "X"),
    (2, 4, 4, "X", "X"),
    (3, 0, 4, "X", "X"),
    (3, 4, 4, "X", "X"),
)
ORDERS = (
    (
        "9:x1",
        "4:x1",
        "1:z0",
        "7:x1",
        "2:x1",
        "5:x1",
        "0:z0",
        "8:x1",
        "6:x1",
        "4:z0",
        "7:z0",
        "2:z0",
        "3:x1",
        "9:z0",
        "5:z0",
        "1:zf",
        "8:z0",
        "6:z0",
        "4:f",
        "0:zf",
        "3:z0",
        "1:f",
        "7:f",
        "7:r1",
        "0:f",
        "2:f",
        "5:r1",
        "5:f",
        "4:r2",
        "2:r2",
        "2:r1",
        "4:r1",
        "9:f",
        "1:b0",
        "8:f",
        "7:r2",
        "5:r2",
        "8:r1",
        "6:f",
        "3:f",
        "9:r2",
        "6:r1",
        "0:b0",
        "8:r2",
        "6:r2",
        "3:r1",
        "5:r3",
        "2:r3",
        "4:r3",
        "9:r3",
        "9:r1",
        "7:r3",
        "8:r3",
        "6:r3",
        "3:r2",
        "3:r3",
    ),
    (
        "4:x1",
        "9:x1",
        "7:x1",
        "5:x1",
        "1:a",
        "1:zf",
        "0:a",
        "1:b",
        "2:x1",
        "8:x1",
        "6:x1",
        "4:a",
        "1:f",
        "7:a",
        "0:b",
        "2:a",
        "9:a",
        "0:zf",
        "4:f",
        "4:b",
        "1:rM",
        "3:x1",
        "5:a",
        "7:b",
        "2:f",
        "9:b",
        "2:b",
        "1:b0",
        "7:f",
        "4:rM",
        "8:a",
        "5:f",
        "5:b",
        "0:f",
        "1:sM",
        "2:rM",
        "6:a",
        "8:f",
        "8:b",
        "5:rM",
        "7:rM",
        "3:a",
        "6:b",
        "9:f",
        "6:f",
        "4:rE",
        "8:rM",
        "5:rE",
        "3:b",
        "9:rM",
        "2:rE",
        "9:rE",
        "3:f",
        "7:rE",
        "8:rE",
        "6:rM",
        "0:b0",
        "2:rF",
        "5:rF",
        "6:rE",
        "4:rF",
        "9:rF",
        "7:rF",
        "1:sE",
        "1:rE",
        "8:rF",
        "3:rE",
        "0:rE",
        "6:rF",
        "3:rM",
        "0:sE",
        "0:sM",
        "3:rF",
        "0:rF",
        "1:rF",
        "0:sF",
        "1:sF",
        "0:rM",
    ),
)


def encode(x, limit):
    power = jnp.exp2(jnp.abs(x) * (2 * SPAN / limit) - SPAN)
    return jnp.where(x < 0, -power, power).astype(jnp.bfloat16)


def decode(code, limit):
    y = code.astype(jnp.float32)
    size = (jnp.log2(jnp.abs(y)) + SPAN) * (limit / (2 * SPAN))
    return jnp.where(y < 0, -size, size)


def kernel(n, kinds, limit, *refs):
    count = len(kinds)
    groups = n // 2
    refs = list(refs)

    def take(k):
        out = refs[:k]
        del refs[:k]
        return out

    source, master = take(count), take(count)
    norm, bias, norm_master, bias_master = take(4)
    gathered, stepped = take(count), take(count)
    vec_all, vec_mine = take(2)
    pair_out, pair_in, part_out, part_in = take(count), take(count), take(count), take(count)
    own, partial = take(count), take(count)
    vec_out, vec_in = take(2)
    (in_sem,) = take(1)
    a_send, a_recv, b_send, b_recv, c_send, c_recv, d_send, d_recv = take(8)
    v_send, v_recv, w_send, w_recv = take(4)

    rate = n ** (-0.5)
    b = lax.axis_index("batch")
    side = lax.rem(b, 2)
    g = b // 2
    partner = b + 1 - 2 * side

    def remote(src, dst, send, recv, to):
        return pltpu.make_async_remote_copy(
            src_ref=src,
            dst_ref=dst,
            send_sem=send,
            recv_sem=recv,
            device_id={"batch": to},
            device_id_type=pl.DeviceIdType.MESH,
        )

    chunks = [(a, h) for h in range(HALVES) for a in range(count)]

    def place(a, h, d):
        rows, cols = stepped[a].shape
        r = rows // HALVES
        if kinds[a] == "rows":
            return pl.ds(pl.multiple_of(d * rows + h * r, r), r), pl.ds(0, cols)
        return pl.ds(h * r, r), pl.ds(pl.multiple_of(d * cols, cols), cols)

    def load(a, h, d):
        rows, cols = place(a, h, d)
        return partial[a][rows, cols]

    def other(k):
        return lax.rem(g + k, groups)

    loads = [
        pltpu.make_async_copy(source[a].at[0], partial[a], in_sem.at[a])
        for a in range(count)
    ]
    for copy in loads:
        copy.start()

    barrier = pltpu.get_barrier_semaphore()
    for k in range(1, n):
        pl.semaphore_signal(
            barrier,
            inc=1,
            device_id={"batch": lax.rem(b + k, n)},
            device_id_type=pl.DeviceIdType.MESH,
        )

    def pair_encode(c):
        a, h = chunks[c]

        def body(k, carry):
            pair_out[a][h, k] = encode(load(a, h, 2 * k + 1 - side), limit)
            return carry

        lax.fori_loop(0, groups, body, 0)

    def pair_copy(c):
        a, h = chunks[c]
        return remote(
            pair_out[a].at[h], pair_in[a].at[h], a_send.at[c], a_recv.at[c], partner
        )

    def part_copy(c, src_slot, dst_slot, to):
        a, h = chunks[c]
        return remote(
            part_out[a].at[h, src_slot],
            part_in[a].at[h, dst_slot],
            b_send.at[c, src_slot],
            b_recv.at[c, dst_slot],
            2 * to + side,
        )

    def pair_finish(c):
        a, h = chunks[c]
        pair_copy(c).wait_recv()
        for k in range(1, groups):
            to = other(k)
            total = load(a, h, 2 * to + side) + decode(pair_in[a][h, to], limit)
            part_out[a][h, to] = encode(total, 2 * limit)
            part_copy(c, to, g, to).start()
        own[a][h] = load(a, h, b) + decode(pair_in[a][h, g], limit)

    def line_copy(c, owner, way, to=None):
        a, h = chunks[c]
        rows, cols = place(a, h, owner)
        block = gathered[a].at[rows, cols]
        return remote(
            block,
            block,
            c_send.at[(way + 1) // 2, c, owner // 2],
            c_recv.at[c, owner // 2],
            b + 2 * way if to is None else to,
        )

    def has_next(way):
        return g < groups - 1 if way > 0 else g > 0

    def has_source(way, k):
        return g - k >= 0 if way > 0 else g + k < groups

    def cross_copy(c, owner, recv_owner):
        a, h = chunks[c]
        rows, cols = place(a, h, owner)
        block = gathered[a].at[rows, cols]
        return remote(
            block, block, d_send.at[c, owner // 2], d_recv.at[c, recv_owner // 2], partner
        )

    def part_finish(c):
        a, h = chunks[c]
        r = stepped[a].shape[0] // HALVES
        total = own[a][h]
        for k in range(1, groups):
            source = other(k)
            part_copy(c, source, source, source).wait_recv()
            total = total + decode(part_in[a][h, source], 2 * limit)
        rows = pl.ds(h * r, r)
        new = master[a][rows, :] - learn_rate * (total * rate)
        stepped[a][rows, :] = new
        at_rows, at_cols = place(a, h, b)
        gathered[a][at_rows, at_cols] = new.astype(jnp.bfloat16)
        for way in (1, -1):

            @pl.when(has_next(way))
            def _():
                line_copy(c, b, way).start()

        cross_copy(c, b, b).start()

    def line_finish(c, k):
        for way in (1, -1):

            @pl.when(has_source(way, k))
            def _():
                owner = b - 2 * k * way
                line_copy(c, owner, way, owner).wait_recv()

                @pl.when(has_next(way))
                def _():
                    line_copy(c, owner, way).start()

                cross_copy(c, owner, owner).start()

    def vec_copy(k):
        to = lax.rem(b + k, n)
        return remote(vec_out.at[to], vec_in.at[b], v_send.at[to], v_recv.at[b], to)

    def vec_back(k):
        to = lax.rem(b + k, n)
        return remote(vec_all.at[b], vec_all.at[b], w_send.at[to], w_recv.at[b], to)

    loads[0].wait()
    pair_encode(0)
    pl.semaphore_wait(barrier, n - 1)
    pair_copy(0).start()
    for d in range(n):
        vec_out[d, 0:1, :] = norm[d]
        vec_out[d, 1:2, :] = bias[d]
    for k in range(1, n):
        vec_copy(k).start()
    for c in range(1, len(chunks)):
        if c < count:
            loads[c].wait()
        pair_encode(c)
        pair_copy(c).start()

    for t in range(len(chunks) + groups):
        if t < len(chunks):
            pair_finish(t)
        if 0 <= t - 1 < len(chunks):
            part_finish(t - 1)
        if t == 1:
            total = vec_out[b]
            for k in range(1, n):
                source = lax.rem(b + k, n)
                remote(
                    vec_out.at[source],
                    vec_in.at[source],
                    v_send.at[source],
                    v_recv.at[source],
                    source,
                ).wait_recv()
                total = total + vec_in[source]
            mean = total * rate
            vec_mine[0:1, :] = norm_master[...] - learn_rate * mean[0:1]
            vec_mine[1:2, :] = bias_master[...] - learn_rate * mean[1:2]
            vec_all[b] = vec_mine[...]
            for k in range(1, n):
                vec_back(k).start()
        for k in range(groups - 1, 0, -1):
            if 0 <= t - 1 - k < len(chunks):
                line_finish(t - 1 - k, k)

    for c in range(len(chunks)):
        for k in range(groups):
            owner = 2 * other(k) + 1 - side
            cross_copy(c, owner, owner).wait_recv()
    for k in range(1, n):
        source = lax.rem(b + k, n)
        remote(
            vec_all.at[source],
            vec_all.at[source],
            w_send.at[source],
            w_recv.at[source],
            source,
        ).wait_recv()
    for k in range(1, n):
        vec_copy(k).wait_send()
        vec_back(k).wait_send()
    for c in range(len(chunks)):
        pair_copy(c).wait_send()
        for k in range(1, groups):
            to = other(k)
            part_copy(c, to, g, to).wait_send()
        for k in range(groups):
            owner = 2 * other(k) + side
            cross_copy(c, owner, owner).wait_send()
        for way in (1, -1):

            @pl.when(has_next(way))
            def _():
                line_copy(c, b, way).wait_send()

            for k in range(1, groups):

                @pl.when(has_source(way, k) & has_next(way))
                def _():
                    line_copy(c, b - 2 * k * way, way).wait_send()


def ladder(n, kinds, limit, plan, orders, *refs):
    count = len(kinds)
    groups = n // 2
    tiny = len(plan) - 1
    refs = list(refs)

    def take(k):
        out = refs[:k]
        del refs[:k]
        return out

    source, master_in = take(count), take(count)
    norm, bias, norm_in, bias_in = take(4)
    gathered, stepped = take(count), take(count)
    norm_out, bias_out, norm_step, bias_step = take(4)
    chunks = len(plan)
    x1_out, x1_in = take(chunks), take(chunks)
    z_out, far_in, near_in = take(chunks), take(chunks), take(chunks)
    x2_out, x2_in, own = take(chunks), take(chunks), take(chunks)
    partial, master = take(count), take(count)
    vec_all, vec_part, norm_part, bias_part, norm_master, bias_master = take(6)
    in_sem, master_sem, small_sem = take(3)
    (tally,) = take(1)
    all_send, leaf_recv, tiny_send, tiny_recv = take(4)
    x1_recv, x2_recv, z_recv, relay_recv = take(4)

    rate = n ** (-0.5)
    b = lax.axis_index("batch")
    side = lax.rem(b, 2)
    g = b // 2
    partner = b + 1 - 2 * side
    way = jnp.where(g < groups // 2, 1, -1)
    is_end = (g == 0) | (g == groups - 1)

    loads = [
        pltpu.make_async_copy(source[a].at[0], partial[a], in_sem.at[a])
        for a in range(count)
    ]
    masters = [
        pltpu.make_async_copy(master_in[a], master[a], master_sem.at[0])
        for a in range(count)
    ]
    smalls = [
        pltpu.make_async_copy(src, dst, small_sem.at[i])
        for i, (src, dst) in enumerate(
            (
                (norm, norm_part),
                (bias, bias_part),
                (norm_in, norm_master),
                (bias_in, bias_master),
            )
        )
    ]

    def remote(src, dst, send, recv, to):
        return pltpu.make_async_remote_copy(
            src_ref=src,
            dst_ref=dst,
            send_sem=send,
            recv_sem=recv,
            device_id={"batch": to},
            device_id_type=pl.DeviceIdType.MESH,
        )

    def place(c, d):
        a, start, size = plan[c][:3]
        rows, cols = stepped[a].shape
        if kinds[a] == "rows":
            return pl.ds(pl.multiple_of(d * rows + start, 16), size), pl.ds(0, cols)
        return pl.ds(start, size), pl.ds(pl.multiple_of(d * cols, cols), cols)

    def load(c, d):
        if c == tiny:
            return vec_part[d]
        rows, cols = place(c, d)
        return partial[plan[c][0]][rows, cols]

    def block(c, d):
        if c == tiny:
            return vec_all.at[d]
        rows, cols = place(c, d)
        return gathered[plan[c][0]].at[rows, cols]

    def pack(c, x, terms):
        return x if c == tiny else encode(x, terms * limit)

    def unpack(c, code, terms):
        return code if c == tiny else decode(code, terms * limit)

    def program(end, order):
        waited = set()
        sent, tiny_sent = [], []
        out_to = b + 2 * way
        near_to = b - 2 * way
        lines = ("out",) if end else ("near", "out")

        def first(key, wait):
            if key not in waited:
                waited.add(key)
                wait()

        def slot(c):
            return tiny_send.at[len(tiny_sent)] if c == tiny else all_send.at[0]

        def send(c, copy):
            if not sent and not tiny_sent:
                pl.semaphore_wait(barrier, 2 if end else 3)
            copy.start()
            (tiny_sent if c == tiny else sent).append(copy)

        def settle(rows):
            ref = tally.at[pl.ds(0, rows)]
            return remote(ref, ref, all_send.at[0], leaf_recv.at[0], partner)

        def x1_copy(c):
            return remote(x1_out[c], x1_in[c], slot(c), x1_recv.at[c], partner)

        def x2_copy(c):
            return remote(x2_out[c], x2_in[c], slot(c), x2_recv.at[c], partner)

        def need(c):
            if c < tiny:
                first(("load", plan[c][0]), loads[plan[c][0]].wait)
                return

            def gather():
                for copy in smalls:
                    copy.wait()
                for d in range(n):
                    vec_part[d, 0:1, :] = norm_part[d]
                    vec_part[d, 1:2, :] = bias_part[d]

            first("small", gather)

        def z_copy(c, kind):
            m = 2 if plan[c][3] == "Z" else 1
            if kind == "end":
                lo, size, dst, to = 0, 3 * m, far_in[c], out_to
            elif kind == "mid":
                dst = near_in[c].at[pl.ds(0, 2 * m)]
                lo, size, to = 0, 2 * m, out_to
            else:
                dst = near_in[c].at[pl.ds(0, m)]
                lo, size, to = 2 * m, m, near_to
            return remote(
                z_out[c].at[pl.ds(lo, size)],
                dst,
                slot(c),
                z_recv.at[0 if kind == "end" else 1, c],
                to,
            )

        def got_far(c):
            first(("far", c), z_copy(c, "end").wait_recv)

        def got_near(c):
            first(("near", c), z_copy(c, "back" if end else "mid").wait_recv)

        def got_x1(c):
            first(("x1", c), x1_copy(c).wait_recv)

        def pair(c, z):
            return load(c, 2 * z + side) + unpack(c, x1_in[c][z], 1)

        def each(lo, hi, fn):
            def body(j, carry):
                fn(j)
                return carry

            lax.fori_loop(lo, hi, body, 0)

        def x1(c):
            need(c)

            def put(z):
                x1_out[c][z] = pack(c, load(c, 2 * z + 1 - side), 1)

            each(0, groups, put)
            send(c, x1_copy(c))

        def z0(c):
            need(c)
            if plan[c][3] == "Z":

                def put(j):
                    d = 2 * (g + way * (j // 2 + 1)) + lax.rem(j, 2)
                    z_out[c][j] = pack(c, load(c, d), 1)

                each(0, 6, put)
            else:
                got_x1(c)

                def put(j):
                    z_out[c][j] = pack(c, pair(c, g + way * (j + 1)), 2)

                each(0, 3, put)
            send(c, z_copy(c, "end"))

        def a(c):
            need(c)
            if plan[c][3] == "Z":
                got_far(c)

                def put(j):
                    d = 2 * (g + way * (j // 2 + 1)) + lax.rem(j, 2)
                    total = load(c, d) + unpack(c, far_in[c][j + 2], 1)
                    z_out[c][j] = pack(c, total, 2)

                each(0, 4, put)
            else:
                got_x1(c)
                got_far(c)

                def put(j):
                    total = pair(c, g + way * (j + 1)) + unpack(c, far_in[c][j + 1], 2)
                    z_out[c][j] = pack(c, total, 4)

                each(0, 2, put)
            send(c, z_copy(c, "mid"))

        def back(c):
            need(c)
            z = g - way
            if plan[c][3] == "Z":
                got_near(c)

                def put(s):
                    total = load(c, 2 * z + s) + unpack(c, near_in[c][2 + s], 2)
                    z_out[c][4 + s] = pack(c, total, 3)

                each(0, 2, put)
            else:
                got_x1(c)
                got_near(c)
                total = pair(c, z) + unpack(c, near_in[c][1], 4)
                z_out[c][2] = pack(c, total, 6)
            send(c, z_copy(c, "back"))

        def line_sum(c, s):
            total = load(c, 2 * g + s)
            if end:
                return total + unpack(c, near_in[c][s], 3)
            return total + unpack(c, far_in[c][s], 1) + unpack(c, near_in[c][s], 2)

        def zf(c):
            need(c)
            got_near(c)
            if not end:
                got_far(c)
            x2_out[c][...] = pack(c, line_sum(c, 1 - side), 4)
            send(c, x2_copy(c))
            own[c][...] = line_sum(c, side)

        def arrival(c, here, step, s):
            if c == tiny:
                return tiny_recv.at[2 * (g + way * step) + (1 - side if s else side)]
            kind = plan[c][4]
            if (kind == "Z" and here) if step or not s else kind != "Z":
                return leaf_recv.at[0]
            if kind != "Z" and s:
                return leaf_recv.at[0]
            base = sum(7 if p[4] == "Z" else 3 for p in plan[:c])
            at = {-1: 0, 1: 1, 2: 2} if not here else {1: 0, 2: 1, 3: 2}
            return relay_recv.at[base + (6 if s and not step else at[step] + 3 * s)]

        def block_copy(c, d, lane, step, s):
            to = {
                "x": partner,
                "out": out_to,
                "near": near_to,
                "two": b + 4 * way,
                "three": b + 6 * way,
            }[lane]
            if lane == "x":
                there, step_there, s_there = end, step, 1 - s
            elif end:
                there = lane == "three"
                step_there, s_there = {"out": -1, "two": 2, "three": 3}[lane], s
            elif lane == "near":
                there, step_there, s_there = True, step + 1, s
            else:
                there = lane == "two"
                step_there, s_there = {"out": 1 - step, "two": 2}[lane], s
            ref = block(c, d)
            if c == tiny:
                recv = tiny_recv.at[d]
            else:
                recv = arrival(c, there, step_there, s_there)
            return remote(ref, ref, slot(c), recv, to)

        def got(c, step, s):
            d = 2 * (g + way * step) + (1 - side if s else side)
            ref = block(c, d)
            copy = remote(ref, ref, slot(c), arrival(c, end, step, s), partner)
            first(("block", c, step, s), copy.wait_recv)
            return d

        def leaf(c, step, s):
            if plan[c][4] == "Z":
                return end and step != 0
            return s == 1

        def f(c):
            need(c)
            if plan[c][3] == "Z":
                x2_copy(c).wait_recv()
                total = own[c][...] + unpack(c, x2_in[c][...], 4)
            else:
                got_x1(c)
                got_near(c)
                total = pair(c, g)
                if end:
                    total = total + unpack(c, near_in[c][0], 6)
                else:
                    got_far(c)
                    total = total + unpack(c, far_in[c][0], 2)
                    total = total + unpack(c, near_in[c][0], 4)
            if c == tiny:
                mean = total * rate
                norm_step[...] = norm_master[...] - learn_rate * mean[0:1]
                bias_step[...] = bias_master[...] - learn_rate * mean[1:2]
                vec_all[b, 0:1, :] = norm_step[...]
                vec_all[b, 1:2, :] = bias_step[...]
            else:
                k, start, size = plan[c][:3]
                half = partial[0].shape[0] // 2
                first("master", lambda: pltpu.make_async_copy(
                    partial[0].at[pl.ds(0, half)],
                    partial[1].at[pl.ds(0, half)],
                    master_sem.at[0],
                ).wait())
                rows = pl.ds(start, size)
                new = master[k][rows, :] - learn_rate * (total * rate)
                stepped[k][rows, :] = new
                at_rows, at_cols = place(c, b)
                gathered[k][at_rows, at_cols] = new.astype(jnp.bfloat16)
            direct = ("three", "two") if end else ("two",)
            for lane in (direct if plan[c][4] == "D" else ()) + lines + ("x",):
                send(c, block_copy(c, b, lane, 0, 0))

        def relay(step, s, lanes):
            def go(c):
                d = got(c, step, s)
                kind = plan[c][4]
                lanes_now = (() if kind == "D" else lanes) + (() if kind == "Z" else ("x",))
                for lane in lanes_now:
                    send(c, block_copy(c, d, lane, step, s))

            return go

        moves = {"x1": x1, "z0": z0, "a": a, "b": back, "zf": zf, "f": f}
        moves["b0"] = relay(0, 1, lines)
        for step in (1, 2, 3):
            moves[f"r{step}"] = relay(step, 0, ())
        for name, step, lane in (("E", -1, "out"), ("M", 1, "near"), ("F", 2, "near")):
            moves["r" + name] = relay(step, 0, (lane,))
            moves["s" + name] = relay(step, 1, (lane,))

        for to in (partner, out_to) if end else (partner, out_to, near_to):
            pl.semaphore_signal(
                barrier,
                inc=1,
                device_id={"batch": to},
                device_id_type=pl.DeviceIdType.MESH,
            )
        for k in dict.fromkeys(plan[c][0] for c, _ in order if c < tiny):
            loads[k].start()
        for copy in smalls + masters:
            copy.start()
        for c, move in order:
            moves[move](c)
        steps = (0, 1, 2, 3) if end else (-1, 0, 1, 2)
        left = [(c, k, s) for c in range(chunks) for k in steps for s in (0, 1) if k or s]
        for c, step, s in left:
            if c == tiny or not leaf(c, step, s):
                got(c, step, s)
        norm_out[...] = vec_all[:, 0, :].astype(jnp.bfloat16)
        bias_out[...] = vec_all[:, 1, :].astype(jnp.bfloat16)
        for copy in tiny_sent:
            copy.wait_send()
        row = tally.shape[1] * 4

        def nbytes(ref):
            return math.prod(ref.shape) * 2

        settle(sum(nbytes(copy.src_ref) for copy in sent) // row).wait_send()
        last = [nbytes(block(c, 0)) for c, step, s in left if c != tiny and leaf(c, step, s)]
        settle(sum(last) // row).wait_recv()

    barrier = pltpu.get_barrier_semaphore()

    @pl.when(is_end)
    def _():
        program(True, orders[0])

    @pl.when(jnp.logical_not(is_end))
    def _():
        program(False, orders[1])


def hand_over(count, *refs):
    sources, vec_all, vec_mine = refs[:count], refs[count], refs[count + 1]
    targets = refs[count + 2 : 2 * count + 2]
    norm, bias, norm_step, bias_step = refs[2 * count + 2 : 2 * count + 6]
    (out_sem,) = refs[2 * count + 6 :]
    outs = [
        pltpu.make_async_copy(sources[i], targets[i], out_sem.at[i]) for i in range(count)
    ]
    for copy in outs:
        copy.start()
    norm[...] = vec_all[:, 0, :].astype(jnp.bfloat16)
    bias[...] = vec_all[:, 1, :].astype(jnp.bfloat16)
    norm_step[...] = vec_mine[0:1, :]
    bias_step[...] = vec_mine[1:2, :]
    for copy in outs:
        copy.wait()


def deliver(count, *refs):
    sources, targets, sem = refs[:count], refs[count:-1], refs[-1]
    copies = []
    for i in range(count):
        rows = sources[i].shape[0]
        pieces = PIECES if rows >= 128 else 1
        for k in range(pieces):
            at = pl.ds(k * (rows // pieces), rows // pieces)
            copies.append(
                pltpu.make_async_copy(sources[i].at[at], targets[i].at[at], sem.at[i, k])
            )
    for copy in copies:
        copy.start()
    for copy in copies:
        copy.wait()


def exchange_ladder(partials, masters, vectors, limit, kinds):
    n = lax.axis_size("batch")
    groups = n // 2
    w = vectors[-1].shape[1]
    plan = []
    for a, start, size, reduce_kind, gather_kind in PLAN:
        rows = masters[a].shape[0]
        plan.append((a, start * rows // 8, size * rows // 8, reduce_kind, gather_kind))
    shapes = [(size, masters[a].shape[1]) for a, _, size, _, _ in plan] + [(2, w)]
    types = [jnp.bfloat16] * len(plan) + [jnp.float32]
    plan.append((None, 0, 2, "X", "X"))
    orders = [
        [(int(c), move) for c, move in (step.split(":") for step in order)]
        for order in ORDERS
    ]

    def buffers(lead):
        return [pltpu.VMEM((*lead(p), *s), t) for p, s, t in zip(plan, shapes, types)]

    def line(k):
        return buffers(lambda p: (2 * k if p[3] == "Z" else k,))

    dma = pltpu.SemaphoreType.DMA
    chunks = len(plan)
    out_shape = [pltpu.VMEM(p.shape[1:], jnp.bfloat16) for p in partials]
    out_shape += [pltpu.VMEM(m.shape, jnp.float32) for m in masters]
    out_shape += [pltpu.VMEM((n, w), jnp.bfloat16)] * 2
    out_shape += [pltpu.VMEM((1, w), jnp.float32)] * 2
    scratch = buffers(lambda p: (groups if p[3] == "X" else 1,)) * 2
    scratch += line(3) * 2 + line(2)
    scratch += buffers(lambda p: ()) * 2
    scratch += [pltpu.VMEM(s, jnp.float32) for s in shapes]
    scratch += [pltpu.VMEM(p.shape[1:], jnp.float32) for p in partials]
    scratch += [pltpu.VMEM(m.shape, jnp.float32) for m in masters]
    scratch += [pltpu.VMEM((n, 2, w), jnp.float32)] * 2
    scratch += [pltpu.VMEM((n, 1, w), jnp.float32)] * 2
    scratch += [pltpu.VMEM((1, w), jnp.float32)] * 2
    rows = 18 * sum(m.size for m in masters) // 512
    scratch += [dma((len(partials),)), dma((1,)), dma((4,))]
    scratch += [pltpu.VMEM((rows, 256), jnp.float32)]
    scratch += [dma((1,)), dma((1,)), dma((12,)), dma((n,))]
    relays = sum(7 if p[4] == "Z" else 3 for p in plan)
    scratch += [dma((chunks,)), dma((chunks,)), dma((2, chunks)), dma((relays,))]
    args = (*partials, *masters, *vectors)
    outs = pl.pallas_call(
        functools.partial(ladder, n, kinds, limit, plan, orders),
        out_shape=out_shape,
        in_specs=[pl.BlockSpec(memory_space=pltpu.HBM)] * len(args),
        out_specs=[pl.BlockSpec(memory_space=pltpu.VMEM)] * len(out_shape),
        scratch_shapes=scratch,
        compiler_params=pltpu.CompilerParams(
            collective_id=0, has_side_effects=True, vmem_limit_bytes=40 << 20
        ),
    )(*(pltpu.with_memory_space_constraint(x, pltpu.HBM) for x in args))
    return pl.pallas_call(
        functools.partial(deliver, len(outs)),
        out_shape=[jax.ShapeDtypeStruct(x.shape, x.dtype) for x in outs],
        in_specs=[pl.BlockSpec(memory_space=pltpu.VMEM)] * len(outs),
        out_specs=[pl.BlockSpec(memory_space=pltpu.HBM)] * len(outs),
        scratch_shapes=[dma((len(outs), PIECES))],
        compiler_params=pltpu.CompilerParams(vmem_limit_bytes=8 << 20),
    )(*(pltpu.with_memory_space_constraint(x, pltpu.VMEM) for x in outs))


def per_device(
    partial_query,
    partial_key,
    partial_value,
    partial_mixed,
    partial_norm,
    partial_bias,
    master_query,
    master_key,
    master_value,
    master_mixed,
    master_norm,
    master_bias,
):
    n = lax.axis_size("batch")
    groups = n // 2
    limit = 0.875 if n <= 8 else 1.25
    wide = master_mixed.shape[1] % 128 == 0
    kinds = ("rows", "rows", "rows", "cols" if wide else "rows")
    if not wide:
        partial_mixed = jnp.swapaxes(partial_mixed, 1, 2)
        master_mixed = master_mixed.T
    partials = (partial_query, partial_key, partial_value, partial_mixed)
    masters = (master_query, master_key, master_value, master_mixed)
    chunk_count = len(partials) * HALVES
    w = master_norm.shape[0]

    out_shape = [jax.ShapeDtypeStruct(p.shape[1:], jnp.bfloat16) for p in partials]
    out_shape += [jax.ShapeDtypeStruct(m.shape, jnp.float32) for m in masters]
    out_shape += [
        jax.ShapeDtypeStruct((n, 2, w), jnp.float32),
        jax.ShapeDtypeStruct((2, w), jnp.float32),
    ]
    coded = [
        pltpu.VMEM((HALVES, groups, m.shape[0] // HALVES, m.shape[1]), jnp.bfloat16)
        for m in masters
    ]
    owns = [
        pltpu.VMEM((HALVES, m.shape[0] // HALVES, m.shape[1]), jnp.float32)
        for m in masters
    ]
    dma = pltpu.SemaphoreType.DMA
    vmem = pl.BlockSpec(memory_space=pltpu.VMEM)
    hbm = pl.BlockSpec(memory_space=pltpu.HBM)
    pin = lambda x: pltpu.with_memory_space_constraint(x, pltpu.HBM)
    exchange = pl.pallas_call(
        functools.partial(kernel, n, kinds, limit),
        out_shape=[pltpu.VMEM(x.shape, x.dtype) for x in out_shape],
        in_specs=[hbm] * len(partials) + [vmem] * (len(partials) + 4),
        out_specs=[vmem] * len(out_shape),
        scratch_shapes=coded * 4
        + owns
        + [pltpu.VMEM(p.shape[1:], jnp.float32) for p in partials]
        + [pltpu.VMEM((n, 2, w), jnp.float32)] * 2
        + [dma((len(partials),))]
        + [dma((chunk_count,))] * 2
        + [dma((chunk_count, groups))] * 2
        + [dma((2, chunk_count, groups))]
        + [dma((chunk_count, groups))] * 3
        + [dma((n,))] * 4,
        compiler_params=pltpu.CompilerParams(collective_id=0, has_side_effects=True, vmem_limit_bytes=40 << 20),
    )
    vectors = (
        partial_norm.reshape(n, 1, w),
        partial_bias.reshape(n, 1, w),
        master_norm.reshape(1, w),
        master_bias.reshape(1, w),
    )
    if n == 8 and wide and all(m.shape[0] % 128 == 0 for m in masters):
        outs = exchange_ladder(partials, masters, vectors, limit, kinds)
    else:
        outs = exchange(*(pin(x) for x in (*partials, *masters, *vectors)))
        large, (vec_all, vec_mine) = outs[:8], outs[8:]
        tail_shape = [jax.ShapeDtypeStruct(x.shape, x.dtype) for x in large]
        tail_shape += [jax.ShapeDtypeStruct((n, w), jnp.bfloat16)] * 2
        tail_shape += [jax.ShapeDtypeStruct((1, w), jnp.float32)] * 2
        outs = pl.pallas_call(
            functools.partial(hand_over, len(large)),
            out_shape=tail_shape,
            in_specs=[vmem] * (len(large) + 2),
            out_specs=[hbm] * len(large) + [vmem] * 4,
            scratch_shapes=[dma((len(large),))],
            compiler_params=pltpu.CompilerParams(vmem_limit_bytes=8 << 20),
        )(*(pltpu.with_memory_space_constraint(x, pltpu.VMEM) for x in (*large, vec_all, vec_mine)))
    computes, steppeds, vectors = outs[:4], outs[4:8], outs[8:]
    if not wide:
        computes = (*computes[:3], computes[3].T)
        steppeds = (*steppeds[:3], steppeds[3].T)
    norm, bias, norm_step, bias_step = (v.reshape(-1) for v in vectors)
    return (*computes, norm, bias, *steppeds, norm_step, bias_step)


def solution(mesh):
    in_specs = (
        P("batch", None, "cols"),
        P("batch", None, "cols"),
        P("batch", None, "cols"),
        P("batch", "cols", None),
        P("batch", None),
        P("batch", None),
        P("batch", "cols"),
        P("batch", "cols"),
        P("batch", "cols"),
        P("cols", "batch"),
        P("batch"),
        P("batch"),
    )
    out_specs = (
        P(None, "cols"),
        P(None, "cols"),
        P(None, "cols"),
        P("cols", None),
        P(),
        P(),
        P("batch", "cols"),
        P("batch", "cols"),
        P("batch", "cols"),
        P("cols", "batch"),
        P("batch"),
        P("batch"),
    )
    return jax.shard_map(
        per_device, mesh=mesh, in_specs=in_specs, out_specs=out_specs, check_vma=False
    )
```

```python
import functools
import math

import jax
import jax.numpy as jnp
from jax import lax
from jax.experimental import pallas as pl
from jax.experimental.pallas import tpu as pltpu
from jax.sharding import PartitionSpec as P

learn_rate = 0.4
HALVES = 2
SPAN = 125.0
PIECES = 2

PLAN = (
    (0, 0, 4, "Z", "Z"),
    (0, 4, 2, "Z", "Z"),
    (0, 6, 2, "X", "X"),
    (1, 0, 4, "X", "X"),
    (1, 4, 4, "X", "X"),
    (2, 0, 4, "X", "X"),
    (2, 4, 4, "X", "X"),
    (3, 0, 4, "X", "X"),
    (3, 4, 4, "X", "X"),
)
ORDERS = (
    (
        "9:x1",
        "4:x1",
        "1:z0",
        "7:x1",
        "2:x1",
        "5:x1",
        "0:z0",
        "8:x1",
        "6:x1",
        "4:z0",
        "7:z0",
        "2:z0",
        "3:x1",
        "9:z0",
        "5:z0",
        "1:zf",
        "8:z0",
        "6:z0",
        "4:f",
        "0:zf",
        "3:z0",
        "1:f",
        "7:f",
        "7:r1",
        "0:f",
        "2:f",
        "5:r1",
        "5:f",
        "4:r2",
        "2:r2",
        "2:r1",
        "4:r1",
        "9:f",
        "1:b0",
        "8:f",
        "7:r2",
        "5:r2",
        "8:r1",
        "6:f",
        "3:f",
        "9:r2",
        "6:r1",
        "0:b0",
        "8:r2",
        "6:r2",
        "3:r1",
        "5:r3",
        "2:r3",
        "4:r3",
        "9:r3",
        "9:r1",
        "7:r3",
        "8:r3",
        "6:r3",
        "3:r2",
        "3:r3",
    ),
    (
        "4:x1",
        "9:x1",
        "7:x1",
        "5:x1",
        "1:a",
        "1:zf",
        "0:a",
        "1:b",
        "2:x1",
        "8:x1",
        "6:x1",
        "4:a",
        "1:f",
        "7:a",
        "0:b",
        "2:a",
        "9:a",
        "0:zf",
        "4:f",
        "4:b",
        "1:rM",
        "3:x1",
        "5:a",
        "7:b",
        "2:f",
        "9:b",
        "2:b",
        "1:b0",
        "7:f",
        "4:rM",
        "8:a",
        "5:f",
        "5:b",
        "0:f",
        "1:sM",
        "2:rM",
        "6:a",
        "8:f",
        "8:b",
        "5:rM",
        "7:rM",
        "3:a",
        "6:b",
        "9:f",
        "6:f",
        "4:rE",
        "8:rM",
        "5:rE",
        "3:b",
        "9:rM",
        "2:rE",
        "9:rE",
        "3:f",
        "7:rE",
        "8:rE",
        "6:rM",
        "0:b0",
        "2:rF",
        "5:rF",
        "6:rE",
        "4:rF",
        "9:rF",
        "7:rF",
        "1:sE",
        "1:rE",
        "8:rF",
        "3:rE",
        "0:rE",
        "6:rF",
        "3:rM",
        "0:sE",
        "0:sM",
        "3:rF",
        "0:rF",
        "1:rF",
        "0:sF",
        "1:sF",
        "0:rM",
    ),
)


def encode(x, limit):
    power = jnp.exp2(jnp.abs(x) * (2 * SPAN / limit) - SPAN)
    return jnp.where(x < 0, -power, power).astype(jnp.bfloat16)


def decode(code, limit):
    y = code.astype(jnp.float32)
    size = (jnp.log2(jnp.abs(y)) + SPAN) * (limit / (2 * SPAN))
    return jnp.where(y < 0, -size, size)


def kernel(n, kinds, limit, *refs):
    count = len(kinds)
    groups = n // 2
    refs = list(refs)

    def take(k):
        out = refs[:k]
        del refs[:k]
        return out

    source, master = take(count), take(count)
    norm, bias, norm_master, bias_master = take(4)
    gathered, stepped = take(count), take(count)
    vec_all, vec_mine = take(2)
    pair_out, pair_in, part_out, part_in = take(count), take(count), take(count), take(count)
    own, partial = take(count), take(count)
    vec_out, vec_in = take(2)
    (in_sem,) = take(1)
    a_send, a_recv, b_send, b_recv, c_send, c_recv, d_send, d_recv = take(8)
    v_send, v_recv, w_send, w_recv = take(4)

    rate = n ** (-0.5)
    b = lax.axis_index("batch")
    side = lax.rem(b, 2)
    g = b // 2
    partner = b + 1 - 2 * side

    def remote(src, dst, send, recv, to):
        return pltpu.make_async_remote_copy(
            src_ref=src,
            dst_ref=dst,
            send_sem=send,
            recv_sem=recv,
            device_id={"batch": to},
            device_id_type=pl.DeviceIdType.MESH,
        )

    chunks = [(a, h) for h in range(HALVES) for a in range(count)]

    def place(a, h, d):
        rows, cols = stepped[a].shape
        r = rows // HALVES
        if kinds[a] == "rows":
            return pl.ds(pl.multiple_of(d * rows + h * r, r), r), pl.ds(0, cols)
        return pl.ds(h * r, r), pl.ds(pl.multiple_of(d * cols, cols), cols)

    def load(a, h, d):
        rows, cols = place(a, h, d)
        return partial[a][rows, cols]

    def other(k):
        return lax.rem(g + k, groups)

    loads = [
        pltpu.make_async_copy(source[a].at[0], partial[a], in_sem.at[a])
        for a in range(count)
    ]
    for copy in loads:
        copy.start()

    barrier = pltpu.get_barrier_semaphore()
    for k in range(1, n):
        pl.semaphore_signal(
            barrier,
            inc=1,
            device_id={"batch": lax.rem(b + k, n)},
            device_id_type=pl.DeviceIdType.MESH,
        )

    def pair_encode(c):
        a, h = chunks[c]

        def body(k, carry):
            pair_out[a][h, k] = encode(load(a, h, 2 * k + 1 - side), limit)
            return carry

        lax.fori_loop(0, groups, body, 0)

    def pair_copy(c):
        a, h = chunks[c]
        return remote(
            pair_out[a].at[h], pair_in[a].at[h], a_send.at[c], a_recv.at[c], partner
        )

    def part_copy(c, src_slot, dst_slot, to):
        a, h = chunks[c]
        return remote(
            part_out[a].at[h, src_slot],
            part_in[a].at[h, dst_slot],
            b_send.at[c, src_slot],
            b_recv.at[c, dst_slot],
            2 * to + side,
        )

    def pair_finish(c):
        a, h = chunks[c]
        pair_copy(c).wait_recv()
        for k in range(1, groups):
            to = other(k)
            total = load(a, h, 2 * to + side) + decode(pair_in[a][h, to], limit)
            part_out[a][h, to] = encode(total, 2 * limit)
            part_copy(c, to, g, to).start()
        own[a][h] = load(a, h, b) + decode(pair_in[a][h, g], limit)

    def line_copy(c, owner, way, to=None):
        a, h = chunks[c]
        rows, cols = place(a, h, owner)
        block = gathered[a].at[rows, cols]
        return remote(
            block,
            block,
            c_send.at[(way + 1) // 2, c, owner // 2],
            c_recv.at[c, owner // 2],
            b + 2 * way if to is None else to,
        )

    def has_next(way):
        return g < groups - 1 if way > 0 else g > 0

    def has_source(way, k):
        return g - k >= 0 if way > 0 else g + k < groups

    def cross_copy(c, owner, recv_owner):
        a, h = chunks[c]
        rows, cols = place(a, h, owner)
        block = gathered[a].at[rows, cols]
        return remote(
            block, block, d_send.at[c, owner // 2], d_recv.at[c, recv_owner // 2], partner
        )

    def part_finish(c):
        a, h = chunks[c]
        r = stepped[a].shape[0] // HALVES
        total = own[a][h]
        for k in range(1, groups):
            source = other(k)
            part_copy(c, source, source, source).wait_recv()
            total = total + decode(part_in[a][h, source], 2 * limit)
        rows = pl.ds(h * r, r)
        new = master[a][rows, :] - learn_rate * (total * rate)
        stepped[a][rows, :] = new
        at_rows, at_cols = place(a, h, b)
        gathered[a][at_rows, at_cols] = new.astype(jnp.bfloat16)
        for way in (1, -1):

            @pl.when(has_next(way))
            def _():
                line_copy(c, b, way).start()

        cross_copy(c, b, b).start()

    def line_finish(c, k):
        for way in (1, -1):

            @pl.when(has_source(way, k))
            def _():
                owner = b - 2 * k * way
                line_copy(c, owner, way, owner).wait_recv()

                @pl.when(has_next(way))
                def _():
                    line_copy(c, owner, way).start()

                cross_copy(c, owner, owner).start()

    def vec_copy(k):
        to = lax.rem(b + k, n)
        return remote(vec_out.at[to], vec_in.at[b], v_send.at[to], v_recv.at[b], to)

    def vec_back(k):
        to = lax.rem(b + k, n)
        return remote(vec_all.at[b], vec_all.at[b], w_send.at[to], w_recv.at[b], to)

    loads[0].wait()
    pair_encode(0)
    pl.semaphore_wait(barrier, n - 1)
    pair_copy(0).start()
    for d in range(n):
        vec_out[d, 0:1, :] = norm[d]
        vec_out[d, 1:2, :] = bias[d]
    for k in range(1, n):
        vec_copy(k).start()
    for c in range(1, len(chunks)):
        if c < count:
            loads[c].wait()
        pair_encode(c)
        pair_copy(c).start()

    for t in range(len(chunks) + groups):
        if t < len(chunks):
            pair_finish(t)
        if 0 <= t - 1 < len(chunks):
            part_finish(t - 1)
        if t == 1:
            total = vec_out[b]
            for k in range(1, n):
                source = lax.rem(b + k, n)
                remote(
                    vec_out.at[source],
                    vec_in.at[source],
                    v_send.at[source],
                    v_recv.at[source],
                    source,
                ).wait_recv()
                total = total + vec_in[source]
            mean = total * rate
            vec_mine[0:1, :] = norm_master[...] - learn_rate * mean[0:1]
            vec_mine[1:2, :] = bias_master[...] - learn_rate * mean[1:2]
            vec_all[b] = vec_mine[...]
            for k in range(1, n):
                vec_back(k).start()
        for k in range(groups - 1, 0, -1):
            if 0 <= t - 1 - k < len(chunks):
                line_finish(t - 1 - k, k)

    for c in range(len(chunks)):
        for k in range(groups):
            owner = 2 * other(k) + 1 - side
            cross_copy(c, owner, owner).wait_recv()
    for k in range(1, n):
        source = lax.rem(b + k, n)
        remote(
            vec_all.at[source],
            vec_all.at[source],
            w_send.at[source],
            w_recv.at[source],
            source,
        ).wait_recv()
    for k in range(1, n):
        vec_copy(k).wait_send()
        vec_back(k).wait_send()
    for c in range(len(chunks)):
        pair_copy(c).wait_send()
        for k in range(1, groups):
            to = other(k)
            part_copy(c, to, g, to).wait_send()
        for k in range(groups):
            owner = 2 * other(k) + side
            cross_copy(c, owner, owner).wait_send()
        for way in (1, -1):

            @pl.when(has_next(way))
            def _():
                line_copy(c, b, way).wait_send()

            for k in range(1, groups):

                @pl.when(has_source(way, k) & has_next(way))
                def _():
                    line_copy(c, b - 2 * k * way, way).wait_send()


def ladder(n, kinds, limit, plan, orders, *refs):
    count = len(kinds)
    groups = n // 2
    tiny = len(plan) - 1
    refs = list(refs)

    def take(k):
        out = refs[:k]
        del refs[:k]
        return out

    source, master_in = take(count), take(count)
    norm, bias, norm_in, bias_in = take(4)
    gathered, stepped = take(count), take(count)
    norm_out, bias_out, norm_step, bias_step = take(4)
    chunks = len(plan)
    x1_out, x1_in = take(chunks), take(chunks)
    z_out, far_in, near_in = take(chunks), take(chunks), take(chunks)
    x2_out, x2_in, own = take(chunks), take(chunks), take(chunks)
    partial, master = take(count), take(count)
    vec_all, vec_part, norm_part, bias_part, norm_master, bias_master = take(6)
    in_sem, master_sem, small_sem = take(3)
    (tally,) = take(1)
    all_send, leaf_recv, tiny_send, tiny_recv = take(4)
    x1_recv, x2_recv, z_recv, relay_recv = take(4)

    rate = n ** (-0.5)
    b = lax.axis_index("batch")
    side = lax.rem(b, 2)
    g = b // 2
    partner = b + 1 - 2 * side
    way = jnp.where(g < groups // 2, 1, -1)
    is_end = (g == 0) | (g == groups - 1)

    loads = [
        pltpu.make_async_copy(source[a].at[0], partial[a], in_sem.at[a])
        for a in range(count)
    ]
    masters = [
        pltpu.make_async_copy(master_in[a], master[a], master_sem.at[0])
        for a in range(count)
    ]
    smalls = [
        pltpu.make_async_copy(src, dst, small_sem.at[i])
        for i, (src, dst) in enumerate(
            (
                (norm, norm_part),
                (bias, bias_part),
                (norm_in, norm_master),
                (bias_in, bias_master),
            )
        )
    ]

    def remote(src, dst, send, recv, to):
        return pltpu.make_async_remote_copy(
            src_ref=src,
            dst_ref=dst,
            send_sem=send,
            recv_sem=recv,
            device_id={"batch": to},
            device_id_type=pl.DeviceIdType.MESH,
        )

    def place(c, d):
        a, start, size = plan[c][:3]
        rows, cols = stepped[a].shape
        if kinds[a] == "rows":
            return pl.ds(pl.multiple_of(d * rows + start, 16), size), pl.ds(0, cols)
        return pl.ds(start, size), pl.ds(pl.multiple_of(d * cols, cols), cols)

    def load(c, d):
        if c == tiny:
            return vec_part[d]
        rows, cols = place(c, d)
        return partial[plan[c][0]][rows, cols]

    def block(c, d):
        if c == tiny:
            return vec_all.at[d]
        rows, cols = place(c, d)
        return gathered[plan[c][0]].at[rows, cols]

    def pack(c, x, terms):
        return x if c == tiny else encode(x, terms * limit)

    def unpack(c, code, terms):
        return code if c == tiny else decode(code, terms * limit)

    def program(end, order):
        waited = set()
        sent, tiny_sent = [], []
        out_to = b + 2 * way
        near_to = b - 2 * way
        lines = ("out",) if end else ("near", "out")

        def first(key, wait):
            if key not in waited:
                waited.add(key)
                wait()

        def slot(c):
            return tiny_send.at[len(tiny_sent)] if c == tiny else all_send.at[0]

        def send(c, copy):
            if not sent and not tiny_sent:
                pl.semaphore_wait(barrier, 2 if end else 3)
            copy.start()
            (tiny_sent if c == tiny else sent).append(copy)

        def settle(rows):
            ref = tally.at[pl.ds(0, rows)]
            return remote(ref, ref, all_send.at[0], leaf_recv.at[0], partner)

        def x1_copy(c):
            return remote(x1_out[c], x1_in[c], slot(c), x1_recv.at[c], partner)

        def x2_copy(c):
            at = sum(p[3] == "Z" for p in plan[:c])
            return remote(x2_out[c], x2_in[c], slot(c), x2_recv.at[at], partner)

        def need(c):
            if c < tiny:
                first(("load", plan[c][0]), loads[plan[c][0]].wait)
                return

            def gather():
                for copy in smalls:
                    copy.wait()
                for d in range(n):
                    vec_part[d, 0:1, :] = norm_part[d]
                    vec_part[d, 1:2, :] = bias_part[d]

            first("small", gather)

        def z_copy(c, kind):
            m = 2 if plan[c][3] == "Z" else 1
            if kind == "end":
                lo, size, dst, to = 0, 3 * m, far_in[c], out_to
            elif kind == "mid":
                dst = near_in[c].at[pl.ds(0, 2 * m)]
                lo, size, to = 0, 2 * m, out_to
            else:
                dst = near_in[c].at[pl.ds(0, m)]
                lo, size, to = 2 * m, m, near_to
            return remote(
                z_out[c].at[pl.ds(lo, size)],
                dst,
                slot(c),
                z_recv.at[0 if kind == "end" else 1, c],
                to,
            )

        def got_far(c):
            first(("far", c), z_copy(c, "end").wait_recv)

        def got_near(c):
            first(("near", c), z_copy(c, "back" if end else "mid").wait_recv)

        def got_x1(c):
            first(("x1", c), x1_copy(c).wait_recv)

        def pair(c, z):
            return load(c, 2 * z + side) + unpack(c, x1_in[c][z], 1)

        def each(lo, hi, fn):
            def body(j, carry):
                fn(j)
                return carry

            lax.fori_loop(lo, hi, body, 0)

        def x1(c):
            need(c)

            def put(z):
                x1_out[c][z] = pack(c, load(c, 2 * z + 1 - side), 1)

            each(0, groups, put)
            send(c, x1_copy(c))

        def z0(c):
            need(c)
            if plan[c][3] == "Z":

                def put(j):
                    d = 2 * (g + way * (j // 2 + 1)) + lax.rem(j, 2)
                    z_out[c][j] = pack(c, load(c, d), 1)

                each(0, 6, put)
            else:
                got_x1(c)

                def put(j):
                    z_out[c][j] = pack(c, pair(c, g + way * (j + 1)), 2)

                each(0, 3, put)
            send(c, z_copy(c, "end"))

        def a(c):
            need(c)
            if plan[c][3] == "Z":
                got_far(c)

                def put(j):
                    d = 2 * (g + way * (j // 2 + 1)) + lax.rem(j, 2)
                    total = load(c, d) + unpack(c, far_in[c][j + 2], 1)
                    z_out[c][j] = pack(c, total, 2)

                each(0, 4, put)
            else:
                got_x1(c)
                got_far(c)

                def put(j):
                    total = pair(c, g + way * (j + 1)) + unpack(c, far_in[c][j + 1], 2)
                    z_out[c][j] = pack(c, total, 4)

                each(0, 2, put)
            send(c, z_copy(c, "mid"))

        def back(c):
            need(c)
            z = g - way
            if plan[c][3] == "Z":
                got_near(c)

                def put(s):
                    total = load(c, 2 * z + s) + unpack(c, near_in[c][2 + s], 2)
                    z_out[c][4 + s] = pack(c, total, 3)

                each(0, 2, put)
            else:
                got_x1(c)
                got_near(c)
                total = pair(c, z) + unpack(c, near_in[c][1], 4)
                z_out[c][2] = pack(c, total, 6)
            send(c, z_copy(c, "back"))

        def line_sum(c, s):
            total = load(c, 2 * g + s)
            if end:
                return total + unpack(c, near_in[c][s], 3)
            return total + unpack(c, far_in[c][s], 1) + unpack(c, near_in[c][s], 2)

        def zf(c):
            need(c)
            got_near(c)
            if not end:
                got_far(c)
            x2_out[c][...] = pack(c, line_sum(c, 1 - side), 4)
            send(c, x2_copy(c))
            own[c][...] = line_sum(c, side)

        def arrival(c, here, step, s):
            if c == tiny:
                return tiny_recv.at[2 * (g + way * step) + (1 - side if s else side)]
            kind = plan[c][4]
            if (kind == "Z" and here) if step or not s else kind != "Z":
                return leaf_recv.at[0]
            if kind != "Z" and s:
                return leaf_recv.at[0]
            base = sum(7 if p[4] == "Z" else 3 for p in plan[:c])
            at = {-1: 0, 1: 1, 2: 2} if not here else {1: 0, 2: 1, 3: 2}
            return relay_recv.at[base + (6 if s and not step else at[step] + 3 * s)]

        def block_copy(c, d, lane, step, s):
            to = {
                "x": partner,
                "out": out_to,
                "near": near_to,
                "two": b + 4 * way,
                "three": b + 6 * way,
            }[lane]
            if lane == "x":
                there, step_there, s_there = end, step, 1 - s
            elif end:
                there = lane == "three"
                step_there, s_there = {"out": -1, "two": 2, "three": 3}[lane], s
            elif lane == "near":
                there, step_there, s_there = True, step + 1, s
            else:
                there = lane == "two"
                step_there, s_there = {"out": 1 - step, "two": 2}[lane], s
            ref = block(c, d)
            if c == tiny:
                recv = tiny_recv.at[d]
            else:
                recv = arrival(c, there, step_there, s_there)
            return remote(ref, ref, slot(c), recv, to)

        def got(c, step, s):
            d = 2 * (g + way * step) + (1 - side if s else side)
            ref = block(c, d)
            copy = remote(ref, ref, slot(c), arrival(c, end, step, s), partner)
            first(("block", c, step, s), copy.wait_recv)
            return d

        def leaf(c, step, s):
            if plan[c][4] == "Z":
                return end and step != 0
            return s == 1

        def f(c):
            need(c)
            if plan[c][3] == "Z":
                x2_copy(c).wait_recv()
                total = own[c][...] + unpack(c, x2_in[c][...], 4)
            else:
                got_x1(c)
                got_near(c)
                total = pair(c, g)
                if end:
                    total = total + unpack(c, near_in[c][0], 6)
                else:
                    got_far(c)
                    total = total + unpack(c, far_in[c][0], 2)
                    total = total + unpack(c, near_in[c][0], 4)
            if c == tiny:
                mean = total * rate
                norm_step[...] = norm_master[...] - learn_rate * mean[0:1]
                bias_step[...] = bias_master[...] - learn_rate * mean[1:2]
                vec_all[b, 0:1, :] = norm_step[...]
                vec_all[b, 1:2, :] = bias_step[...]
            else:
                k, start, size = plan[c][:3]
                half = partial[0].shape[0] // 2
                first("master", lambda: pltpu.make_async_copy(
                    partial[0].at[pl.ds(0, half)],
                    partial[1].at[pl.ds(0, half)],
                    master_sem.at[0],
                ).wait())
                rows = pl.ds(start, size)
                new = master[k][rows, :] - learn_rate * (total * rate)
                stepped[k][rows, :] = new
                at_rows, at_cols = place(c, b)
                gathered[k][at_rows, at_cols] = new.astype(jnp.bfloat16)
            direct = ("three", "two") if end else ("two",)
            for lane in (direct if plan[c][4] == "D" else ()) + lines + ("x",):
                send(c, block_copy(c, b, lane, 0, 0))

        def relay(step, s, lanes):
            def go(c):
                d = got(c, step, s)
                kind = plan[c][4]
                lanes_now = (() if kind == "D" else lanes) + (() if kind == "Z" else ("x",))
                for lane in lanes_now:
                    send(c, block_copy(c, d, lane, step, s))

            return go

        moves = {"x1": x1, "z0": z0, "a": a, "b": back, "zf": zf, "f": f}
        moves["b0"] = relay(0, 1, lines)
        for step in (1, 2, 3):
            moves[f"r{step}"] = relay(step, 0, ())
        for name, step, lane in (("E", -1, "out"), ("M", 1, "near"), ("F", 2, "near")):
            moves["r" + name] = relay(step, 0, (lane,))
            moves["s" + name] = relay(step, 1, (lane,))

        for to in (partner, out_to) if end else (partner, out_to, near_to):
            pl.semaphore_signal(
                barrier,
                inc=1,
                device_id={"batch": to},
                device_id_type=pl.DeviceIdType.MESH,
            )
        for k in dict.fromkeys(plan[c][0] for c, _ in order if c < tiny):
            loads[k].start()
        for copy in smalls + masters:
            copy.start()
        for c, move in order:
            moves[move](c)
        steps = (0, 1, 2, 3) if end else (-1, 0, 1, 2)
        left = [(c, k, s) for c in range(chunks) for k in steps for s in (0, 1) if k or s]
        for c, step, s in left:
            if c == tiny or not leaf(c, step, s):
                got(c, step, s)
        norm_out[...] = vec_all[:, 0, :].astype(jnp.bfloat16)
        bias_out[...] = vec_all[:, 1, :].astype(jnp.bfloat16)
        for copy in tiny_sent:
            copy.wait_send()
        row = tally.shape[1] * 4

        def nbytes(ref):
            return math.prod(ref.shape) * 2

        settle(sum(nbytes(copy.src_ref) for copy in sent) // row).wait_send()
        last = [nbytes(block(c, 0)) for c, step, s in left if c != tiny and leaf(c, step, s)]
        settle(sum(last) // row).wait_recv()

    barrier = pltpu.get_barrier_semaphore()

    @pl.when(is_end)
    def _():
        program(True, orders[0])

    @pl.when(jnp.logical_not(is_end))
    def _():
        program(False, orders[1])


def hand_over(count, *refs):
    sources, vec_all, vec_mine = refs[:count], refs[count], refs[count + 1]
    targets = refs[count + 2 : 2 * count + 2]
    norm, bias, norm_step, bias_step = refs[2 * count + 2 : 2 * count + 6]
    (out_sem,) = refs[2 * count + 6 :]
    outs = [
        pltpu.make_async_copy(sources[i], targets[i], out_sem.at[i]) for i in range(count)
    ]
    for copy in outs:
        copy.start()
    norm[...] = vec_all[:, 0, :].astype(jnp.bfloat16)
    bias[...] = vec_all[:, 1, :].astype(jnp.bfloat16)
    norm_step[...] = vec_mine[0:1, :]
    bias_step[...] = vec_mine[1:2, :]
    for copy in outs:
        copy.wait()


def deliver(large, count, *refs):
    sources, targets = refs[:count], refs[count : 2 * count]
    tally, sem = refs[2 * count :]
    copies = []
    for i in range(count):
        rows = sources[i].shape[0]
        pieces = PIECES if i < large else 1
        for k in range(pieces):
            at = pl.ds(k * (rows // pieces), rows // pieces)
            which = 0 if i < large else 1 + i - large
            copies.append(
                pltpu.make_async_copy(sources[i].at[at], targets[i].at[at], sem.at[which])
            )
    for copy in copies:
        copy.start()
    for copy in copies[large * PIECES :]:
        copy.wait()
    pltpu.make_async_copy(tally, tally, sem.at[0]).wait()


def exchange_ladder(partials, masters, vectors, limit, kinds):
    n = lax.axis_size("batch")
    groups = n // 2
    w = vectors[-1].shape[1]
    plan = []
    for a, start, size, reduce_kind, gather_kind in PLAN:
        rows = masters[a].shape[0]
        plan.append((a, start * rows // 8, size * rows // 8, reduce_kind, gather_kind))
    shapes = [(size, masters[a].shape[1]) for a, _, size, _, _ in plan] + [(2, w)]
    types = [jnp.bfloat16] * len(plan) + [jnp.float32]
    plan.append((None, 0, 2, "X", "X"))
    orders = [
        [(int(c), move) for c, move in (step.split(":") for step in order)]
        for order in ORDERS
    ]

    def buffers(lead):
        return [pltpu.VMEM((*lead(p), *s), t) for p, s, t in zip(plan, shapes, types)]

    def line(k):
        return buffers(lambda p: (2 * k if p[3] == "Z" else k,))

    dma = pltpu.SemaphoreType.DMA
    chunks = len(plan)
    out_shape = [pltpu.VMEM(p.shape[1:], jnp.bfloat16) for p in partials]
    out_shape += [pltpu.VMEM(m.shape, jnp.float32) for m in masters]
    out_shape += [pltpu.VMEM((n, w), jnp.bfloat16)] * 2
    out_shape += [pltpu.VMEM((1, w), jnp.float32)] * 2
    scratch = buffers(lambda p: (groups if p[3] == "X" else 1,)) * 2
    scratch += line(3) * 2 + line(2)
    scratch += buffers(lambda p: ()) * 2
    scratch += [pltpu.VMEM(s, jnp.float32) for s in shapes]
    scratch += [pltpu.VMEM(p.shape[1:], jnp.float32) for p in partials]
    scratch += [pltpu.VMEM(m.shape, jnp.float32) for m in masters]
    scratch += [pltpu.VMEM((n, 2, w), jnp.float32)] * 2
    scratch += [pltpu.VMEM((n, 1, w), jnp.float32)] * 2
    scratch += [pltpu.VMEM((1, w), jnp.float32)] * 2
    rows = 18 * sum(m.size for m in masters) // 512
    scratch += [dma((len(partials),)), dma((1,)), dma((4,))]
    scratch += [pltpu.VMEM((rows, 256), jnp.float32)]
    scratch += [dma((1,)), dma((1,)), dma((12,)), dma((n,))]
    relays = sum(7 if p[4] == "Z" else 3 for p in plan)
    crossed = max(1, sum(p[3] == "Z" for p in plan))
    scratch += [dma((chunks,)), dma((crossed,)), dma((2, chunks)), dma((relays,))]
    args = (*partials, *masters, *vectors)
    outs = pl.pallas_call(
        functools.partial(ladder, n, kinds, limit, plan, orders),
        out_shape=out_shape,
        in_specs=[pl.BlockSpec(memory_space=pltpu.HBM)] * len(args),
        out_specs=[pl.BlockSpec(memory_space=pltpu.VMEM)] * len(out_shape),
        scratch_shapes=scratch,
        compiler_params=pltpu.CompilerParams(
            collective_id=0, has_side_effects=True, vmem_limit_bytes=40 << 20
        ),
    )(*(pltpu.with_memory_space_constraint(x, pltpu.HBM) for x in args))
    large = 2 * len(partials)
    rows = sum(math.prod(x.shape) * x.dtype.itemsize for x in outs[:large]) // 1024
    return pl.pallas_call(
        functools.partial(deliver, large, len(outs)),
        out_shape=[jax.ShapeDtypeStruct(x.shape, x.dtype) for x in outs],
        in_specs=[pl.BlockSpec(memory_space=pltpu.VMEM)] * len(outs),
        out_specs=[pl.BlockSpec(memory_space=pltpu.HBM)] * len(outs),
        scratch_shapes=[pltpu.VMEM((rows, 256), jnp.float32), dma((5,))],
        compiler_params=pltpu.CompilerParams(vmem_limit_bytes=8 << 20),
    )(*(pltpu.with_memory_space_constraint(x, pltpu.VMEM) for x in outs))


def per_device(
    partial_query,
    partial_key,
    partial_value,
    partial_mixed,
    partial_norm,
    partial_bias,
    master_query,
    master_key,
    master_value,
    master_mixed,
    master_norm,
    master_bias,
):
    n = lax.axis_size("batch")
    groups = n // 2
    limit = 0.875 if n <= 8 else 1.25
    wide = master_mixed.shape[1] % 128 == 0
    kinds = ("rows", "rows", "rows", "cols" if wide else "rows")
    if not wide:
        partial_mixed = jnp.swapaxes(partial_mixed, 1, 2)
        master_mixed = master_mixed.T
    partials = (partial_query, partial_key, partial_value, partial_mixed)
    masters = (master_query, master_key, master_value, master_mixed)
    chunk_count = len(partials) * HALVES
    w = master_norm.shape[0]

    out_shape = [jax.ShapeDtypeStruct(p.shape[1:], jnp.bfloat16) for p in partials]
    out_shape += [jax.ShapeDtypeStruct(m.shape, jnp.float32) for m in masters]
    out_shape += [
        jax.ShapeDtypeStruct((n, 2, w), jnp.float32),
        jax.ShapeDtypeStruct((2, w), jnp.float32),
    ]
    coded = [
        pltpu.VMEM((HALVES, groups, m.shape[0] // HALVES, m.shape[1]), jnp.bfloat16)
        for m in masters
    ]
    owns = [
        pltpu.VMEM((HALVES, m.shape[0] // HALVES, m.shape[1]), jnp.float32)
        for m in masters
    ]
    dma = pltpu.SemaphoreType.DMA
    vmem = pl.BlockSpec(memory_space=pltpu.VMEM)
    hbm = pl.BlockSpec(memory_space=pltpu.HBM)
    pin = lambda x: pltpu.with_memory_space_constraint(x, pltpu.HBM)
    exchange = pl.pallas_call(
        functools.partial(kernel, n, kinds, limit),
        out_shape=[pltpu.VMEM(x.shape, x.dtype) for x in out_shape],
        in_specs=[hbm] * len(partials) + [vmem] * (len(partials) + 4),
        out_specs=[vmem] * len(out_shape),
        scratch_shapes=coded * 4
        + owns
        + [pltpu.VMEM(p.shape[1:], jnp.float32) for p in partials]
        + [pltpu.VMEM((n, 2, w), jnp.float32)] * 2
        + [dma((len(partials),))]
        + [dma((chunk_count,))] * 2
        + [dma((chunk_count, groups))] * 2
        + [dma((2, chunk_count, groups))]
        + [dma((chunk_count, groups))] * 3
        + [dma((n,))] * 4,
        compiler_params=pltpu.CompilerParams(collective_id=0, has_side_effects=True, vmem_limit_bytes=40 << 20),
    )
    vectors = (
        partial_norm.reshape(n, 1, w),
        partial_bias.reshape(n, 1, w),
        master_norm.reshape(1, w),
        master_bias.reshape(1, w),
    )
    if n == 8 and wide and all(m.shape[0] % 128 == 0 for m in masters):
        outs = exchange_ladder(partials, masters, vectors, limit, kinds)
    else:
        outs = exchange(*(pin(x) for x in (*partials, *masters, *vectors)))
        large, (vec_all, vec_mine) = outs[:8], outs[8:]
        tail_shape = [jax.ShapeDtypeStruct(x.shape, x.dtype) for x in large]
        tail_shape += [jax.ShapeDtypeStruct((n, w), jnp.bfloat16)] * 2
        tail_shape += [jax.ShapeDtypeStruct((1, w), jnp.float32)] * 2
        outs = pl.pallas_call(
            functools.partial(hand_over, len(large)),
            out_shape=tail_shape,
            in_specs=[vmem] * (len(large) + 2),
            out_specs=[hbm] * len(large) + [vmem] * 4,
            scratch_shapes=[dma((len(large),))],
            compiler_params=pltpu.CompilerParams(vmem_limit_bytes=8 << 20),
        )(*(pltpu.with_memory_space_constraint(x, pltpu.VMEM) for x in (*large, vec_all, vec_mine)))
    computes, steppeds, vectors = outs[:4], outs[4:8], outs[8:]
    if not wide:
        computes = (*computes[:3], computes[3].T)
        steppeds = (*steppeds[:3], steppeds[3].T)
    norm, bias, norm_step, bias_step = (v.reshape(-1) for v in vectors)
    return (*computes, norm, bias, *steppeds, norm_step, bias_step)


def solution(mesh):
    in_specs = (
        P("batch", None, "cols"),
        P("batch", None, "cols"),
        P("batch", None, "cols"),
        P("batch", "cols", None),
        P("batch", None),
        P("batch", None),
        P("batch", "cols"),
        P("batch", "cols"),
        P("batch", "cols"),
        P("cols", "batch"),
        P("batch"),
        P("batch"),
    )
    out_specs = (
        P(None, "cols"),
        P(None, "cols"),
        P(None, "cols"),
        P("cols", None),
        P(),
        P(),
        P("batch", "cols"),
        P("batch", "cols"),
        P("batch", "cols"),
        P("cols", "batch"),
        P("batch"),
        P("batch"),
    )
    return jax.shard_map(
        per_device, mesh=mesh, in_specs=in_specs, out_specs=out_specs, check_vma=False
    )
```
